32 devices in a mesh: fsdp: 4 (over z), ctx: 4 (over x, core), tp: 2 (over y).
Axes of the slice: x: 2, y: 2, z: 4, core: 2. Of those that a mesh axis runs over, the one named last changes fastest.
Arguments:
- layer_input: float32 [4, 4096, 512], P('fsdp', 'ctx'), may hold values from -6 to 6
- out_grad: float32 [4, 4096, 512], P('fsdp', 'ctx'), may hold values from -6 to 6
- lengths: int32 [4], P('fsdp'), may hold values from 1024 to 4096, as said below
- norm_gains: float32 [5, 512], replicated, may hold values from 0.5 to 1.5
- feed_up: bfloat16 [512, 2048], P('fsdp', 'tp'), may hold values from -0.25 to 0.25
- feed_down: bfloat16 [512, 2048], P('fsdp', 'tp'), may hold values from -0.125 to 0.125
- attend_in: bfloat16 [512, 3, 512], P('fsdp', None, 'tp'), may hold values from -0.25 to 0.25
- attend_out: bfloat16 [512, 512], P('fsdp', 'tp'), may hold values from -6 to 6
- mixer_in: bfloat16 [512, 2, 512], P('fsdp', None, 'tp'), may hold values from -0.25 to 0.25
- mixer_out: bfloat16 [512, 512], P('fsdp', 'tp'), may hold values from -0.25 to 0.25
- depth_kernel: float32 [31, 512], P(None, 'tp'), may hold values from -1.5 to 1.5
- batch_norm: float32 [2, 512], P(None, 'tp'), may hold values from 0.5 to 1.5
- final_up: bfloat16 [512, 2048], P('fsdp', 'tp'), may hold values from -0.25 to 0.25
- final_down: bfloat16 [512, 2048], P('fsdp', 'tp'), may hold values from -0.125 to 0.125
Outputs:
- layer_output: float32 [4, 4096, 512], P('fsdp', 'ctx')
- input_grad: float32 [4, 4096, 512], P('fsdp', 'ctx')
- gains_grad: float32 [5, 512], replicated
- feed_up_grad: float32 [512, 2048], P('fsdp', 'tp')
- feed_down_grad: float32 [512, 2048], P('fsdp', 'tp')
- attend_in_grad: float32 [512, 3, 512], P('fsdp', None, 'tp')
- attend_out_grad: float32 [512, 512], P('fsdp', 'tp')
- mixer_in_grad: float32 [512, 2, 512], P('fsdp', None, 'tp')
- mixer_out_grad: float32 [512, 512], P('fsdp', 'tp')
- kernel_grad: float32 [31, 512], P(None, 'tp')
- norm_grad: float32 [2, 512], P(None, 'tp')
- final_up_grad: float32 [512, 2048], P('fsdp', 'tp')
- final_down_grad: float32 [512, 2048], P('fsdp', 'tp')
The draws below stay inside these ranges and needn't reach their ends.
Inputs may be any that keep to these rules, and one draw needn't show every extreme that they name: `lengths`: every utterance has at least a quarter of its 4096 frames, and one of them has all 4096.
All inputs are finite; a program needn't handle non-finite values.
Results may differ from the reference program's by a relative error of at most 0.038.
Values may be sent and summed in bfloat16 or wider, within the bound.
A program may use at most 384 MiB of HBM per device.

```python
import jax
import jax.numpy as jnp
from jax import lax

D = 512
HEADS = 8
HEAD = 64
FF = 2048
KERNEL = 31
SEQS = 4
LEN = 4096


def draw_lengths(key, part):
    first, second = jax.random.split(key)
    drawn = jax.random.randint(first, (SEQS,), LEN // 4, LEN + 1)
    longest = jax.random.randint(second, (), 0, SEQS)
    return jnp.where(jnp.arange(SEQS) == longest, LEN, drawn).astype(jnp.int32)


def steps_of(own_key, dims, cuts, least, high):
    level, own = 1.0, jax.random.fold_in(own_key, 6)
    for dim, shards_of in cuts:
        draws = jnp.exp(jax.random.uniform(jax.random.fold_in(own, dim), (shards_of,), jnp.float32, least / len(cuts), high / len(cuts)))
        level = level * jnp.repeat(draws, dims[dim] // shards_of).reshape([-1 if axis == dim else 1 for axis in range(len(dims))])
    return level


def gaussian(key, dims, scale, bound, cuts=(), kind=jnp.bfloat16):
    factor_of = steps_of(key, dims, cuts, -0.22, 0.18) if cuts else 1.0
    array = jax.random.normal(key, dims, jnp.float32) * scale * factor_of
    return jnp.minimum(jnp.maximum(array, -bound), bound).astype(kind)


def setup_inputs(seed: int = 0) -> dict:
    key_list = jax.random.split(jax.random.key(seed), 15)
    return {
        "layer_input": gaussian(key_list[0], (SEQS, LEN, D), 1.0, 6.0, ((0, 4), (1, 4)), jnp.float32),
        "out_grad": gaussian(key_list[1], (SEQS, LEN, D), 1.0, 6.0, ((0, 4), (1, 4)), jnp.float32),
        "lengths": draw_lengths(jax.random.fold_in(key_list[14], 71), 0),
        "norm_gains": jnp.clip(1.0 + 0.1 * jax.random.normal(key_list[3], (5, D), jnp.float32), 0.5, 1.5),
        "feed_up": gaussian(key_list[4], (D, FF), D ** -0.5, 0.25, ((0, 4), (1, 2))),
        "feed_down": gaussian(key_list[5], (D, FF), FF ** -0.5, 0.125, ((0, 4), (1, 2))),
        "attend_in": gaussian(key_list[6], (D, 3, D), D ** -0.5, 0.25, ((0, 4), (2, 2))),
        "attend_out": gaussian(key_list[7], (D, D), 1.5, 6.0, ((0, 4), (1, 2))),
        "mixer_in": gaussian(key_list[8], (D, 2, D), D ** -0.5, 0.25, ((0, 4), (2, 2))),
        "mixer_out": gaussian(key_list[9], (D, D), D ** -0.5, 0.25, ((0, 4), (1, 2))),
        "depth_kernel": gaussian(key_list[10], (KERNEL, D), 0.3, 1.5, ((1, 2),), jnp.float32),
        "batch_norm": jnp.clip(0.5 + 1.0 * jax.random.uniform(key_list[11], (2, D), jnp.float32) ** steps_of(key_list[11], (2, D), ((1, 2),), -0.2, 0.2), 0.5, 1.5),
        "final_up": gaussian(key_list[12], (D, FF), D ** -0.5, 0.25, ((0, 4), (1, 2))),
        "final_down": gaussian(key_list[13], (D, FF), FF ** -0.5, 0.125, ((0, 4), (1, 2))),
    }


@jax.custom_vjp
def low(v):
    return lax.optimization_barrier(v.astype(jnp.bfloat16)).astype(jnp.float32)

@jax.custom_vjp
def low_back(v):
    return v

def low_keep(v):
    return (low(v), None)

def low_pass(kept, grad):
    return (grad,)

def back_keep(v):
    return (v, None)

def back_low(kept, grad):
    return (low(grad),)
low.defvjp(low_keep, low_pass)
low_back.defvjp(back_keep, back_low)
norm_eps = 1e-05
masked_score = -1000000000.0
highest = lax.Precision.HIGHEST

def layer_norm(values, gain):
    center = values - lax.optimization_barrier(jnp.mean(values, -1, keepdims=True))
    spread = lax.optimization_barrier(jnp.mean(center * center, -1, keepdims=True))
    return center * lax.rsqrt(spread + norm_eps) * gain

def rotary(values, position):
    half = values.shape[-1] // 2
    inverse = 10000.0 ** (-2.0 * jnp.arange(half, dtype=jnp.float32) / values.shape[-1])
    angle = position.astype(jnp.float32)[:, None] * inverse[None, :]
    cosine = jnp.cos(angle)[:, None, :]
    sine = jnp.sin(angle)[:, None, :]
    lower = values[..., :half]
    upper = values[..., half:]
    return jnp.concatenate([lower * cosine - upper * sine, lower * sine + upper * cosine], -1)

def swish(values):
    return values * jax.nn.sigmoid(values)

def feed(stream, gain, weight_up, weight_down):
    normed = low(layer_norm(stream, gain))
    hidden = low_back(jnp.einsum('bld,df->blf', normed, weight_up, precision=highest))
    active = low(swish(hidden))
    return low_back(jnp.einsum('blf,df->bld', active, weight_down, precision=highest))

def attend_one(inputs):
    query, keys, values, length = inputs
    scores = low_back(jnp.einsum('fhe,lhe->hfl', query, keys, precision=highest))
    live_keys = jnp.arange(LEN) < length
    scores = jnp.where(live_keys[None, None, :], scores, masked_score)
    top = lax.optimization_barrier(jnp.max(scores, -1, keepdims=True))
    raised = jnp.exp(scores - top)
    probs = low(raised / lax.optimization_barrier(jnp.sum(raised, -1, keepdims=True)))
    return low(low_back(jnp.einsum('hfl,lhe->fhe', probs, values, precision=highest)))

def attend(stream, gain, weight_in, weight_out, lengths):
    normed = low(layer_norm(stream, gain))
    projected = low_back(jnp.einsum('bld,dke->blke', normed, weight_in, precision=highest))
    split = projected.reshape(projected.shape[0], LEN, 3, HEADS, HEAD)
    place = jnp.arange(LEN)
    query = low(rotary(split[:, :, 0], place) * HEAD ** (-0.5))
    keys = low(rotary(split[:, :, 1], place))
    values = low(split[:, :, 2])
    mixed = lax.map(jax.checkpoint(attend_one), (query, keys, values, lengths))
    mixed = mixed.reshape(mixed.shape[0], LEN, D)
    return low_back(jnp.einsum('ble,de->bld', mixed, weight_out, precision=highest))

def mixer(stream, gain, weight_in, kernel, norm_params, weight_out, live):
    normed = low(layer_norm(stream, gain))
    gates = low_back(jnp.einsum('bld,dke->blke', normed, weight_in, precision=highest))
    gated = low(gates[:, :, 0] * jax.nn.sigmoid(gates[:, :, 1]) * live[:, :, None])
    reach = KERNEL // 2
    padded = jnp.pad(gated, ((0, 0), (reach, reach), (0, 0)))
    filtered = jnp.zeros_like(gated)
    for offset in range(KERNEL):
        filtered = filtered + kernel[offset] * padded[:, offset:offset + LEN]
    filtered = low_back(filtered)
    mask = live[:, :, None]
    count = jnp.sum(live)
    mean = lax.optimization_barrier(jnp.sum(mask * filtered, (0, 1))) / count
    variance = lax.optimization_barrier(jnp.sum(mask * filtered * filtered, (0, 1))) / count - mean * mean
    unit = (filtered - mean) * lax.rsqrt(variance + norm_eps)
    shifted = unit * norm_params[0] + norm_params[1]
    active = low(swish(shifted))
    return low_back(jnp.einsum('blc,dc->bld', active, weight_out, precision=highest))

def reference(layer_input, out_grad, lengths, norm_gains, feed_up, feed_down, attend_in, attend_out, mixer_in, mixer_out, depth_kernel, batch_norm, final_up, final_down):
    live = (jnp.arange(LEN)[None, :] < lengths[:, None]).astype(jnp.float32)

    def forward(stream, gains, up_one, down_one, proj_in, proj_out, conv_in, conv_out, kernel, norm_params, up_two, down_two):
        after_one = stream + 0.5 * feed(stream, gains[0], up_one, down_one)
        after_two = after_one + attend(after_one, gains[1], proj_in, proj_out, lengths)
        after_three = after_two + mixer(after_two, gains[2], conv_in, kernel, norm_params, conv_out, live)
        after_four = after_three + 0.5 * feed(after_three, gains[3], up_two, down_two)
        return layer_norm(after_four, gains[4])
    result, backward = jax.vjp(forward, layer_input, norm_gains, feed_up.astype(jnp.float32), feed_down.astype(jnp.float32), attend_in.astype(jnp.float32), attend_out.astype(jnp.float32), mixer_in.astype(jnp.float32), mixer_out.astype(jnp.float32), depth_kernel, batch_norm, final_up.astype(jnp.float32), final_down.astype(jnp.float32))
    grads = backward(out_grad)
    return (result, grads[0], grads[1], grads[2], grads[3], grads[4], grads[5], grads[6], grads[7], grads[8], grads[9], grads[10], grads[11])
```

```python
import jax
import jax.numpy as jnp
from jax import lax
from jax.experimental import pallas as pl
from jax.experimental.pallas import tpu as pltpu
from jax.sharding import PartitionSpec as P

HEAD = 64
PAIR = 128
KERNEL = 31


norm_eps = 1e-05
masked_score = -1000000000.0


def split_heads(block, axis):
    spot = lax.broadcasted_iota(jnp.int32, block.shape, axis)
    zero = jnp.zeros_like(block)
    return (jnp.where(spot < HEAD, block, zero), jnp.where(spot < HEAD, zero, block))


def key_bias(length, chunk):
    spot = pl.program_id(1) * chunk + lax.broadcasted_iota(jnp.int32, (chunk, 1), 0)
    return jnp.where(spot < length, 0.0, masked_score)


def attend_forward_kernel(length_ref, q_ref, k_ref, v_ref, o_ref, lse_ref, qt_s, top_s, sum_s):
    chunk = k_ref.shape[0]
    step = pl.program_id(1)

    @pl.when(step == 0)
    def _():
        first, second = split_heads(q_ref[...].T, 0)
        qt_s[0] = first
        qt_s[1] = second
        top_s[...] = jnp.full_like(top_s, -jnp.inf)
        sum_s[...] = jnp.zeros_like(sum_s)
        o_ref[...] = jnp.zeros_like(o_ref)

    bias = key_bias(length_ref[0], chunk)
    values = v_ref[...].T
    for j in range(2):
        scores = jnp.dot(k_ref[...], qt_s[j], preferred_element_type=jnp.float32) + bias
        old = top_s[j]
        top = jnp.maximum(old, jnp.max(scores, 0, keepdims=True))
        fade = jnp.exp(old - top)
        raised = jnp.exp(scores - top)
        top_s[j] = top
        sum_s[j] = sum_s[j] * fade + jnp.sum(raised, 0, keepdims=True)
        rows = slice(j * HEAD, (j + 1) * HEAD)
        o_ref[rows] = o_ref[rows] * fade + jnp.dot(
            values[rows], raised.astype(jnp.bfloat16), preferred_element_type=jnp.float32
        )

    @pl.when(step == pl.num_programs(1) - 1)
    def _():
        for j in range(2):
            rows = slice(j * HEAD, (j + 1) * HEAD)
            o_ref[rows] = o_ref[rows] / sum_s[j]
            lse_ref[j] = top_s[j] + jnp.log(sum_s[j])


def attend_forward(query, joined, length, chunk=512):
    frames, width = query.shape
    keys = joined.shape[0]
    pairs = width // PAIR
    return pl.pallas_call(
        attend_forward_kernel,
        grid_spec=pltpu.PrefetchScalarGridSpec(
            num_scalar_prefetch=1,
            grid=(pairs, keys // chunk),
            in_specs=[
                pl.BlockSpec((frames, PAIR), lambda p, c, n: (0, p)),
                pl.BlockSpec((chunk, PAIR), lambda p, c, n: (c, p)),
                pl.BlockSpec((chunk, PAIR), lambda p, c, n: (c, pairs + p)),
            ],
            out_specs=[
                pl.BlockSpec((PAIR, frames), lambda p, c, n: (p, 0)),
                pl.BlockSpec((2, 1, frames), lambda p, c, n: (p, 0, 0)),
            ],
            scratch_shapes=[
                pltpu.VMEM((2, PAIR, frames), jnp.bfloat16),
                pltpu.VMEM((2, 1, frames), jnp.float32),
                pltpu.VMEM((2, 1, frames), jnp.float32),
            ],
        ),
        out_shape=[
            jax.ShapeDtypeStruct((width, frames), jnp.float32),
            jax.ShapeDtypeStruct((2 * pairs, 1, frames), jnp.float32),
        ],
        compiler_params=pltpu.CompilerParams(vmem_limit_bytes=50 * 1024 * 1024),
        cost_estimate=pl.CostEstimate(
            flops=4 * frames * keys * width,
            bytes_accessed=4 * keys * width + 6 * frames * width,
            transcendentals=2 * pairs * frames * keys,
        ),
        name="attend_forward",
    )(length, query, joined, joined)


def attend_backward_kernel(
    length_ref, q_ref, g_ref, o_ref, lse_ref, k_ref, v_ref, dq_ref, dkv_ref,
    qt_s, gt_s, q_s, g_s, delta_s,
):
    chunk = k_ref.shape[0]

    @pl.when(pl.program_id(1) == 0)
    def _():
        query, grad = q_ref[...], g_ref[...]
        for j, part in enumerate(split_heads(query, 1)):
            q_s[j] = part
        for j, part in enumerate(split_heads(grad, 1)):
            g_s[j] = part
        grad_t = grad.T
        for j, part in enumerate(split_heads(query.T, 0)):
            qt_s[j] = part
        for j, part in enumerate(split_heads(grad_t, 0)):
            gt_s[j] = part
        product = grad_t.astype(jnp.float32) * o_ref[...]
        for j in range(2):
            delta_s[j] = jnp.sum(product[j * HEAD : (j + 1) * HEAD], 0, keepdims=True)
        dq_ref[...] = jnp.zeros_like(dq_ref)

    bias = key_bias(length_ref[0], chunk)
    keys_t = k_ref[...].T
    dk = dv = None
    for j in range(2):
        scores = jnp.dot(k_ref[...], qt_s[j], preferred_element_type=jnp.float32) + bias
        probs = jnp.exp(scores - lse_ref[j])
        dp = jnp.dot(v_ref[...], gt_s[j], preferred_element_type=jnp.float32)
        ds = (probs * (dp - delta_s[j])).astype(jnp.bfloat16)
        dv_j = jnp.dot(probs.astype(jnp.bfloat16), g_s[j], preferred_element_type=jnp.float32)
        dk_j = jnp.dot(ds, q_s[j], preferred_element_type=jnp.float32)
        dk = dk_j if dk is None else dk + dk_j
        dv = dv_j if dv is None else dv + dv_j
        rows = slice(j * HEAD, (j + 1) * HEAD)
        dq_ref[rows] += jnp.dot(keys_t[rows], ds, preferred_element_type=jnp.float32)
    dkv_ref[0] = dk.astype(jnp.bfloat16)
    dkv_ref[1] = dv.astype(jnp.bfloat16)


def attend_backward(query, joined, length, lse, mixed, grad, chunk=512):
    frames, width = query.shape
    keys = joined.shape[0]
    pairs = width // PAIR
    return pl.pallas_call(
        attend_backward_kernel,
        grid_spec=pltpu.PrefetchScalarGridSpec(
            num_scalar_prefetch=1,
            grid=(pairs, keys // chunk),
            in_specs=[
                pl.BlockSpec((frames, PAIR), lambda p, c, n: (0, p)),
                pl.BlockSpec((frames, PAIR), lambda p, c, n: (0, p)),
                pl.BlockSpec((PAIR, frames), lambda p, c, n: (p, 0)),
                pl.BlockSpec((2, 1, frames), lambda p, c, n: (p, 0, 0)),
                pl.BlockSpec((chunk, PAIR), lambda p, c, n: (c, p)),
                pl.BlockSpec((chunk, PAIR), lambda p, c, n: (c, pairs + p)),
            ],
            out_specs=[
                pl.BlockSpec((PAIR, frames), lambda p, c, n: (p, 0)),
                pl.BlockSpec((2, chunk, PAIR), lambda p, c, n: (0, c, p)),
            ],
            scratch_shapes=[
                pltpu.VMEM((2, PAIR, frames), jnp.bfloat16),
                pltpu.VMEM((2, PAIR, frames), jnp.bfloat16),
                pltpu.VMEM((2, frames, PAIR), jnp.bfloat16),
                pltpu.VMEM((2, frames, PAIR), jnp.bfloat16),
                pltpu.VMEM((2, 1, frames), jnp.float32),
            ],
        ),
        out_shape=[
            jax.ShapeDtypeStruct((width, frames), jnp.float32),
            jax.ShapeDtypeStruct((2, keys, width), jnp.bfloat16),
        ],
        compiler_params=pltpu.CompilerParams(vmem_limit_bytes=50 * 1024 * 1024),
        cost_estimate=pl.CostEstimate(
            flops=10 * frames * keys * width,
            bytes_accessed=8 * keys * width + 12 * frames * width,
            transcendentals=2 * pairs * frames * keys,
        ),
        name="attend_backward",
    )(length, query, grad, mixed, lse, joined, joined)


def with_halo(cells, sides, width):
    for axis, dim in sides:
        count = lax.axis_size(axis)
        ends = count - 1
        head = lax.slice_in_dim(cells, 0, width, axis=dim)
        tail = lax.slice_in_dim(cells, cells.shape[dim] - width, cells.shape[dim], axis=dim)
        cells = jnp.concatenate(
            [
                lax.ppermute(tail, axis, [(i, (i + 1) % count) for i in range(ends)]),
                cells,
                lax.ppermute(head, axis, [((i + 1) % count, i) for i in range(ends)]),
            ],
            axis=dim,
        )
    return cells


def layer_norm(values, gain):
    center = values - jnp.mean(values, -1, keepdims=True)
    spread = jnp.mean(center * center, -1, keepdims=True)
    return center * lax.rsqrt(spread + norm_eps) * gain


def rotary(values, position):
    half = values.shape[-1] // 2
    inverse = 10000.0 ** (-2.0 * jnp.arange(half, dtype=jnp.float32) / values.shape[-1])
    angle = position.astype(jnp.float32)[:, None] * inverse[None, :]
    cosine = jnp.cos(angle)[:, None, :]
    sine = jnp.sin(angle)[:, None, :]
    lower = values[..., :half]
    upper = values[..., half:]
    return jnp.concatenate([lower * cosine - upper * sine, lower * sine + upper * cosine], -1)


def swish(values):
    return values * jax.nn.sigmoid(values)


def tensor_total(partial_value):
    low = partial_value.astype(jnp.bfloat16)
    if lax.axis_size("tp") != 2:
        return lax.psum(low, "tp").astype(jnp.float32)
    other = lax.ppermute(low, "tp", [(0, 1), (1, 0)])
    return low.astype(jnp.float32) + other.astype(jnp.float32)


def gather_weights(*shards):
    rows = shards[0].shape[0]
    flat = jnp.concatenate([shard.reshape(rows, -1) for shard in shards], 1)
    part = rows // lax.axis_size("ctx")
    mine = lax.dynamic_slice_in_dim(flat, lax.axis_index("ctx") * part, part, 0)
    whole = lax.all_gather(mine, ("fsdp", "ctx"), axis=0, tiled=True)
    pieces, start = [], 0
    for shard in shards:
        width = shard.size // rows
        pieces.append(
            lax.slice_in_dim(whole, start, start + width, axis=1).reshape(-1, *shard.shape[1:])
        )
        start += width
    return pieces


def pack_grads(*grads):
    return jnp.concatenate(
        [grad.astype(jnp.bfloat16).reshape(grad.shape[0], -1) for grad in grads], 1
    )


def reduce_grads(packed, *shapes):
    part = lax.psum_scatter(packed, ("fsdp", "ctx"), scatter_dimension=0, tiled=True)
    whole = lax.all_gather(part, "ctx", axis=0, tiled=True)
    pieces, start = [], 0
    for shape in shapes:
        width = 1
        for size in shape[1:]:
            width *= size
        pieces.append(
            lax.slice_in_dim(whole, start, start + width, axis=1)
            .astype(jnp.float32)
            .reshape(-1, *shape[1:])
        )
        start += width
    return pieces


def attend_all(query_low, joined_all, lengths):
    batch, frames, heads, _ = query_low.shape
    if (heads * HEAD) % PAIR:
        return lax.map(attend_one, (query_low, joined_all, lengths))
    mixed, totals = [], []
    for row in range(batch):
        out, total = attend_forward(
            query_low[row].reshape(frames, -1), joined_all[row], lengths[row : row + 1]
        )
        mixed.append(out)
        totals.append(total)
    return (jnp.stack(mixed), jnp.stack(totals))


def attend_all_back(query_low, joined_all, lengths, log_total, mixed, mixed_grad):
    batch, frames, heads, _ = query_low.shape
    if (heads * HEAD) % PAIR:
        query_grad, joined_grad = lax.map(
            attend_back, (query_low, joined_all, lengths, log_total, mixed_grad)
        )
        width = heads * HEAD
        low = joined_grad.astype(jnp.bfloat16)
        return (query_grad, jnp.stack([low[..., :width], low[..., width:]], 1))
    queries, others = [], []
    for row in range(batch):
        query_grad, joined_grad = attend_backward(
            query_low[row].reshape(frames, -1),
            joined_all[row],
            lengths[row : row + 1],
            log_total[row],
            mixed[row],
            mixed_grad[row].reshape(frames, -1),
        )
        queries.append(query_grad.T.reshape(frames, heads, HEAD))
        others.append(joined_grad)
    return (jnp.stack(queries), jnp.stack(others))


def product_rows(left, right):
    return lax.dot_general(
        left, right, (((1,), (1,)), ((), ())), preferred_element_type=jnp.float32
    )


def product_cols(left, right):
    return lax.dot_general(
        left, right, (((0,), (0,)), ((), ())), preferred_element_type=jnp.float32
    )


def feed_forward(stream, gain, weight_up, weight_down):
    normed, norm_back = jax.vjp(layer_norm, stream, gain)
    normed_low = normed.astype(jnp.bfloat16)
    hidden = jnp.dot(normed_low, weight_up, preferred_element_type=jnp.float32)
    active, active_back = jax.vjp(swish, hidden)
    active_low = active.astype(jnp.bfloat16)
    branch = tensor_total(product_rows(active_low, weight_down))
    return (branch, (norm_back, normed_low, active_back, active_low))


def feed_backward(branch_grad, saved, weight_up, weight_down):
    norm_back, normed_low, active_back, active_low = saved
    grad_low = branch_grad.astype(jnp.bfloat16)
    down_grad = product_cols(grad_low, active_low)
    hidden_grad = active_back(jnp.dot(grad_low, weight_down, preferred_element_type=jnp.float32))[
        0
    ].astype(jnp.bfloat16)
    up_grad = product_cols(normed_low, hidden_grad)
    normed_grad = tensor_total(product_rows(hidden_grad, weight_up))
    stream_grad, gain_grad = norm_back(normed_grad)
    return (stream_grad, gain_grad, up_grad, down_grad)


def split_joined(joined, heads):
    width = heads * HEAD
    keys = joined[:, :width].reshape(joined.shape[0], heads, HEAD)
    values = joined[:, width:].reshape(joined.shape[0], heads, HEAD)
    return (keys, values)


def attend_scores(query, keys, length):
    scores = jnp.einsum("fhe,lhe->hfl", query, keys, preferred_element_type=jnp.float32)
    live_keys = jnp.arange(keys.shape[0]) < length
    return jnp.where(live_keys[None, None, :], scores, masked_score)


def attend_one(inputs):
    query, joined, length = inputs
    keys, values = split_joined(joined, query.shape[1])
    scores = attend_scores(query, keys, length)
    top = jnp.max(scores, -1, keepdims=True)
    raised = jnp.exp(scores - top)
    total = jnp.sum(raised, -1, keepdims=True)
    weights = (raised / total).astype(jnp.bfloat16)
    mixed = jnp.einsum("hfl,lhe->fhe", weights, values, preferred_element_type=jnp.float32)
    return (mixed.astype(jnp.bfloat16), (top + jnp.log(total))[..., 0])


def attend_back(inputs):
    query, joined, length, log_total, mixed_grad = inputs
    keys, values = split_joined(joined, query.shape[1])
    scores = attend_scores(query, keys, length)
    probs = jnp.exp(scores - log_total[..., None])
    probs_grad = jnp.einsum("fhe,lhe->hfl", mixed_grad, values, preferred_element_type=jnp.float32)
    center = jnp.sum(probs * probs_grad, -1, keepdims=True)
    score_grad = (probs * (probs_grad - center)).astype(jnp.bfloat16)
    query_grad = jnp.einsum("hfl,lhe->fhe", score_grad, keys, preferred_element_type=jnp.float32)
    keys_grad = jnp.einsum("hfl,fhe->lhe", score_grad, query, preferred_element_type=jnp.float32)
    values_grad = jnp.einsum(
        "hfl,fhe->lhe", probs.astype(jnp.bfloat16), mixed_grad, preferred_element_type=jnp.float32
    )
    frames_all = keys.shape[0]
    joined_grad = jnp.concatenate(
        [keys_grad.reshape(frames_all, -1), values_grad.reshape(frames_all, -1)], -1
    )
    return (query_grad, joined_grad)


def per_device(
    layer_input,
    out_grad,
    lengths,
    norm_gains,
    feed_up,
    feed_down,
    attend_in,
    attend_out,
    mixer_in,
    mixer_out,
    depth_kernel,
    batch_norm,
    final_up,
    final_down,
):
    batch, frames, width = layer_input.shape
    rows = batch * frames
    place = lax.axis_index("ctx") * frames + jnp.arange(frames, dtype=jnp.int32)
    live = (place[None, :] < lengths[:, None]).astype(jnp.float32)
    live_rows = live.reshape(rows, 1)
    live_cube = live[:, :, None]
    up_one, down_one = gather_weights(feed_up, feed_down)
    proj_in, proj_out, conv_in, conv_out = gather_weights(
        attend_in, attend_out, mixer_in, mixer_out
    )
    up_two, down_two = gather_weights(final_up, final_down)
    stream = layer_input.reshape(rows, width)
    cotangent = out_grad.reshape(rows, width)
    branch_one, saved_one = feed_forward(stream, norm_gains[0], up_one, down_one)
    after_one = stream + 0.5 * branch_one
    normed, norm_back_two = jax.vjp(layer_norm, after_one, norm_gains[1])
    normed_two = normed.astype(jnp.bfloat16)
    projected = jnp.einsum("nd,dke->nke", normed_two, proj_in, preferred_element_type=jnp.float32)
    local_width = projected.shape[2]
    heads = local_width // HEAD
    split = projected.reshape(batch, frames, 3, heads, HEAD)

    def rotate_pair(query_raw, key_raw):
        return (rotary(query_raw, place) * HEAD ** (-0.5), rotary(key_raw, place))

    (query_rot, key_rot), rotate_back = jax.vjp(rotate_pair, split[:, :, 0], split[:, :, 1])
    query_low = query_rot.astype(jnp.bfloat16)
    joined = jnp.concatenate(
        [
            key_rot.astype(jnp.bfloat16).reshape(batch, frames, local_width),
            split[:, :, 2].astype(jnp.bfloat16).reshape(batch, frames, local_width),
        ],
        -1,
    )
    joined_all = lax.all_gather(joined, "ctx", axis=1, tiled=True)
    mixed, log_total = attend_all(query_low, joined_all, lengths)
    if local_width % PAIR:
        mixed_rows = mixed.reshape(rows, local_width)
    else:
        mixed_rows = mixed.astype(jnp.bfloat16).transpose(0, 2, 1).reshape(rows, local_width)
    after_two = after_one + tensor_total(product_rows(mixed_rows, proj_out))
    normed, norm_back_three = jax.vjp(layer_norm, after_two, norm_gains[2])
    normed_three = normed.astype(jnp.bfloat16)
    gates = jnp.einsum("nd,dke->nke", normed_three, conv_in, preferred_element_type=jnp.float32)

    def gate_linear(values):
        return values[:, 0] * jax.nn.sigmoid(values[:, 1]) * live_rows

    gated, gate_back = jax.vjp(gate_linear, gates)
    channels = gated.shape[1]
    gated_low = gated.astype(jnp.bfloat16).reshape(batch, frames, channels)
    reach = KERNEL // 2
    padded = with_halo(gated_low, (("ctx", 1),), reach)
    filtered = jnp.zeros((batch, frames, channels), jnp.float32)
    for offset in range(KERNEL):
        filtered = filtered + depth_kernel[offset] * padded[:, offset : offset + frames].astype(
            jnp.float32
        )
    sums = lax.psum(
        (
            jnp.sum(live_cube * filtered, (0, 1)),
            jnp.sum(live_cube * filtered * filtered, (0, 1)),
            jnp.sum(live),
        ),
        ("fsdp", "ctx"),
    )
    count = sums[2]
    mean = sums[0] / count
    variance = sums[1] / count - mean * mean
    rescale = lax.rsqrt(variance + norm_eps)
    unit = (filtered - mean) * rescale
    shifted = unit * batch_norm[0] + batch_norm[1]
    active, active_back = jax.vjp(swish, shifted.reshape(rows, channels))
    active_low = active.astype(jnp.bfloat16)
    after_three = after_two + tensor_total(product_rows(active_low, conv_out))
    branch_four, saved_four = feed_forward(after_three, norm_gains[3], up_two, down_two)
    after_four = after_three + 0.5 * branch_four
    result, final_back = jax.vjp(layer_norm, after_four, norm_gains[4])
    grad_four, gain_five = final_back(cotangent)
    stream_grad, gain_four, up_two_grad, down_two_grad = feed_backward(
        0.5 * grad_four, saved_four, up_two, down_two
    )
    grad_three = grad_four + stream_grad
    branch_low = grad_three.astype(jnp.bfloat16)
    conv_out_grad = product_cols(branch_low, active_low)
    shifted_grad = active_back(jnp.dot(branch_low, conv_out, preferred_element_type=jnp.float32))[
        0
    ].reshape(batch, frames, channels)
    bias_sum, scale_sum = lax.psum(
        (jnp.sum(shifted_grad, (0, 1)), jnp.sum(shifted_grad * unit, (0, 1))), ("fsdp", "ctx")
    )
    var_grad = -0.5 * rescale * rescale * batch_norm[0] * scale_sum
    first_grad = (-rescale * batch_norm[0] * bias_sum - 2.0 * mean * var_grad) / count
    second_grad = var_grad / count
    filtered_grad = (
        rescale * batch_norm[0] * shifted_grad
        + live_cube * (first_grad + 2.0 * filtered * second_grad)
    ).astype(jnp.bfloat16)
    padded_grad = with_halo(filtered_grad, (("ctx", 1),), reach)
    filtered_wide = filtered_grad.astype(jnp.float32)
    gated_grad = jnp.zeros((batch, frames, channels), jnp.float32)
    kernel_terms = []
    for offset in range(KERNEL):
        start = 2 * reach - offset
        gated_grad = gated_grad + depth_kernel[offset] * padded_grad[
            :, start : start + frames
        ].astype(jnp.float32)
        kernel_terms.append(
            jnp.sum(filtered_wide * padded[:, offset : offset + frames].astype(jnp.float32), (0, 1))
        )
    kernel_local = jnp.stack(kernel_terms)
    gates_grad = gate_back(gated_grad.reshape(rows, channels))[0].astype(jnp.bfloat16)
    conv_in_grad = jnp.einsum(
        "nd,nke->dke", normed_three, gates_grad, preferred_element_type=jnp.float32
    )
    normed_grad = tensor_total(
        jnp.einsum("nke,dke->nd", gates_grad, conv_in, preferred_element_type=jnp.float32)
    )
    stream_grad, gain_three = norm_back_three(normed_grad)
    grad_two = grad_three + stream_grad
    branch_low = grad_two.astype(jnp.bfloat16)
    proj_out_grad = product_cols(branch_low, mixed_rows)
    mixed_grad = (
        jnp.dot(branch_low, proj_out, preferred_element_type=jnp.float32)
        .astype(jnp.bfloat16)
        .reshape(batch, frames, heads, HEAD)
    )
    early = pack_grads(up_two_grad, down_two_grad, conv_in_grad, conv_out_grad, proj_out_grad)
    early, mixed_grad = lax.optimization_barrier((early, mixed_grad))
    up_two_grad, down_two_grad, conv_in_grad, conv_out_grad, proj_out_grad = reduce_grads(
        early, final_up.shape, final_down.shape, mixer_in.shape, mixer_out.shape, attend_out.shape
    )
    query_grad, joined_grad = attend_all_back(
        query_low, joined_all, lengths, log_total, mixed, mixed_grad
    )
    joined_local = lax.psum_scatter(
        joined_grad, "ctx", scatter_dimension=2, tiled=True
    ).astype(jnp.float32)
    key_grad = joined_local[:, 0].reshape(batch, frames, heads, HEAD)
    value_grad = joined_local[:, 1].reshape(batch, frames, heads, HEAD)
    query_raw_grad, key_raw_grad = rotate_back((query_grad, key_grad))
    proj_grad = (
        jnp.stack([query_raw_grad, key_raw_grad, value_grad], 2)
        .reshape(rows, 3, local_width)
        .astype(jnp.bfloat16)
    )
    proj_in_grad = jnp.einsum(
        "nd,nke->dke", normed_two, proj_grad, preferred_element_type=jnp.float32
    )
    normed_grad = tensor_total(
        jnp.einsum("nke,dke->nd", proj_grad, proj_in, preferred_element_type=jnp.float32)
    )
    stream_grad, gain_two = norm_back_two(normed_grad)
    grad_one = grad_two + stream_grad
    stream_grad, gain_one, up_one_grad, down_one_grad = feed_backward(
        0.5 * grad_one, saved_one, up_one, down_one
    )
    input_grad = grad_one + stream_grad
    gain_terms = jnp.stack([gain_one, gain_two, gain_three, gain_four, gain_five])
    gain_total, kernel_total = lax.psum((gain_terms, kernel_local), ("fsdp", "ctx"))
    up_one_grad, down_one_grad, proj_in_grad = reduce_grads(
        pack_grads(up_one_grad, down_one_grad, proj_in_grad),
        feed_up.shape,
        feed_down.shape,
        attend_in.shape,
    )
    return (
        result.reshape(batch, frames, width),
        input_grad.reshape(batch, frames, width),
        gain_total,
        up_one_grad,
        down_one_grad,
        proj_in_grad,
        proj_out_grad,
        conv_in_grad,
        conv_out_grad,
        kernel_total,
        jnp.stack([scale_sum, bias_sum]),
        up_two_grad,
        down_two_grad,
    )


def solution(mesh):
    placed = (
        P("fsdp", "ctx", None),
        P("fsdp", "ctx", None),
        P("fsdp"),
        P(),
        P("fsdp", "tp"),
        P("fsdp", "tp"),
        P("fsdp", None, "tp"),
        P("fsdp", "tp"),
        P("fsdp", None, "tp"),
        P("fsdp", "tp"),
        P(None, "tp"),
        P(None, "tp"),
        P("fsdp", "tp"),
        P("fsdp", "tp"),
    )
    return jax.shard_map(
        per_device,
        mesh=mesh,
        in_specs=placed,
        out_specs=(
            P("fsdp", "ctx", None),
            P("fsdp", "ctx", None),
            P(),
            P("fsdp", "tp"),
            P("fsdp", "tp"),
            P("fsdp", None, "tp"),
            P("fsdp", "tp"),
            P("fsdp", None, "tp"),
            P("fsdp", "tp"),
            P(None, "tp"),
            P(None, "tp"),
            P("fsdp", "tp"),
            P("fsdp", "tp"),
        ),
        check_vma=False,
    )
```

```python
import functools

import jax
import jax.numpy as jnp
from jax import lax
from jax.experimental import pallas as pl
from jax.experimental.pallas import tpu as pltpu
from jax.sharding import PartitionSpec as P

HEAD = 64
PAIR = 128
KERNEL = 31


norm_eps = 1e-05
masked_score = -1000000000.0


def split_heads(block, axis):
    spot = lax.broadcasted_iota(jnp.int32, block.shape, axis)
    zero = jnp.zeros_like(block)
    return (jnp.where(spot < HEAD, block, zero), jnp.where(spot < HEAD, zero, block))


def key_bias(length, chunk):
    spot = pl.program_id(1) * chunk + lax.broadcasted_iota(jnp.int32, (chunk, 1), 0)
    return jnp.where(spot < length, 0.0, masked_score)


def attend_forward_kernel(length_ref, q_ref, k_ref, v_ref, o_ref, lse_ref, qt_s, top_s, sum_s):
    chunk = k_ref.shape[0]
    step = pl.program_id(1)

    @pl.when(step == 0)
    def _():
        first, second = split_heads(q_ref[...].T, 0)
        qt_s[0] = first
        qt_s[1] = second
        top_s[...] = jnp.full_like(top_s, -jnp.inf)
        sum_s[...] = jnp.zeros_like(sum_s)
        o_ref[...] = jnp.zeros_like(o_ref)

    bias = key_bias(length_ref[0], chunk)
    values = v_ref[...].T
    for j in range(2):
        scores = jnp.dot(k_ref[...], qt_s[j], preferred_element_type=jnp.float32) + bias
        old = top_s[j]
        top = jnp.maximum(old, jnp.max(scores, 0, keepdims=True))
        fade = jnp.exp(old - top)
        raised = jnp.exp(scores - top)
        top_s[j] = top
        sum_s[j] = sum_s[j] * fade + jnp.sum(raised, 0, keepdims=True)
        rows = slice(j * HEAD, (j + 1) * HEAD)
        o_ref[rows] = o_ref[rows] * fade + jnp.dot(
            values[rows], raised.astype(jnp.bfloat16), preferred_element_type=jnp.float32
        )

    @pl.when(step == pl.num_programs(1) - 1)
    def _():
        for j in range(2):
            rows = slice(j * HEAD, (j + 1) * HEAD)
            o_ref[rows] = o_ref[rows] / sum_s[j]
            lse_ref[j] = top_s[j] + jnp.log(sum_s[j])


def attend_forward(query, joined, length, chunk=512):
    frames, width = query.shape
    keys = joined.shape[0]
    pairs = width // PAIR
    return pl.pallas_call(
        attend_forward_kernel,
        grid_spec=pltpu.PrefetchScalarGridSpec(
            num_scalar_prefetch=1,
            grid=(pairs, keys // chunk),
            in_specs=[
                pl.BlockSpec((frames, PAIR), lambda p, c, n: (0, p)),
                pl.BlockSpec((chunk, PAIR), lambda p, c, n: (c, p)),
                pl.BlockSpec((chunk, PAIR), lambda p, c, n: (c, pairs + p)),
            ],
            out_specs=[
                pl.BlockSpec((PAIR, frames), lambda p, c, n: (p, 0)),
                pl.BlockSpec((2, 1, frames), lambda p, c, n: (p, 0, 0)),
            ],
            scratch_shapes=[
                pltpu.VMEM((2, PAIR, frames), jnp.bfloat16),
                pltpu.VMEM((2, 1, frames), jnp.float32),
                pltpu.VMEM((2, 1, frames), jnp.float32),
            ],
        ),
        out_shape=[
            jax.ShapeDtypeStruct((width, frames), jnp.float32),
            jax.ShapeDtypeStruct((2 * pairs, 1, frames), jnp.float32),
        ],
        compiler_params=pltpu.CompilerParams(vmem_limit_bytes=50 * 1024 * 1024),
        cost_estimate=pl.CostEstimate(
            flops=4 * frames * keys * width,
            bytes_accessed=4 * keys * width + 6 * frames * width,
            transcendentals=2 * pairs * frames * keys,
        ),
        name="attend_forward",
    )(length, query, joined, joined)


def attend_backward_kernel(
    length_ref, q_ref, g_ref, o_ref, lse_ref, k_ref, v_ref, dq_ref, dkv_ref,
    qt_s, gt_s, q_s, g_s, delta_s,
):
    chunk = k_ref.shape[0]

    @pl.when(pl.program_id(1) == 0)
    def _():
        query, grad = q_ref[...], g_ref[...]
        for j, part in enumerate(split_heads(query, 1)):
            q_s[j] = part
        for j, part in enumerate(split_heads(grad, 1)):
            g_s[j] = part
        grad_t = grad.T
        for j, part in enumerate(split_heads(query.T, 0)):
            qt_s[j] = part
        for j, part in enumerate(split_heads(grad_t, 0)):
            gt_s[j] = part
        product = grad_t.astype(jnp.float32) * o_ref[...]
        for j in range(2):
            delta_s[j] = jnp.sum(product[j * HEAD : (j + 1) * HEAD], 0, keepdims=True)
        dq_ref[...] = jnp.zeros_like(dq_ref)

    bias = key_bias(length_ref[0], chunk)
    keys_t = k_ref[...].T
    dk = dv = None
    for j in range(2):
        scores = jnp.dot(k_ref[...], qt_s[j], preferred_element_type=jnp.float32) + bias
        probs = jnp.exp(scores - lse_ref[j])
        dp = jnp.dot(v_ref[...], gt_s[j], preferred_element_type=jnp.float32)
        ds = (probs * (dp - delta_s[j])).astype(jnp.bfloat16)
        dv_j = jnp.dot(probs.astype(jnp.bfloat16), g_s[j], preferred_element_type=jnp.float32)
        dk_j = jnp.dot(ds, q_s[j], preferred_element_type=jnp.float32)
        dk = dk_j if dk is None else dk + dk_j
        dv = dv_j if dv is None else dv + dv_j
        rows = slice(j * HEAD, (j + 1) * HEAD)
        dq_ref[rows] += jnp.dot(keys_t[rows], ds, preferred_element_type=jnp.float32)
    dkv_ref[0] = dk.astype(jnp.bfloat16)
    dkv_ref[1] = dv.astype(jnp.bfloat16)


def attend_backward(query, joined, length, lse, mixed, grad, chunk=512):
    frames, width = query.shape
    keys = joined.shape[0]
    pairs = width // PAIR
    return pl.pallas_call(
        attend_backward_kernel,
        grid_spec=pltpu.PrefetchScalarGridSpec(
            num_scalar_prefetch=1,
            grid=(pairs, keys // chunk),
            in_specs=[
                pl.BlockSpec((frames, PAIR), lambda p, c, n: (0, p)),
                pl.BlockSpec((frames, PAIR), lambda p, c, n: (0, p)),
                pl.BlockSpec((PAIR, frames), lambda p, c, n: (p, 0)),
                pl.BlockSpec((2, 1, frames), lambda p, c, n: (p, 0, 0)),
                pl.BlockSpec((chunk, PAIR), lambda p, c, n: (c, p)),
                pl.BlockSpec((chunk, PAIR), lambda p, c, n: (c, pairs + p)),
            ],
            out_specs=[
                pl.BlockSpec((PAIR, frames), lambda p, c, n: (p, 0)),
                pl.BlockSpec((2, chunk, PAIR), lambda p, c, n: (0, c, p)),
            ],
            scratch_shapes=[
                pltpu.VMEM((2, PAIR, frames), jnp.bfloat16),
                pltpu.VMEM((2, PAIR, frames), jnp.bfloat16),
                pltpu.VMEM((2, frames, PAIR), jnp.bfloat16),
                pltpu.VMEM((2, frames, PAIR), jnp.bfloat16),
                pltpu.VMEM((2, 1, frames), jnp.float32),
            ],
        ),
        out_shape=[
            jax.ShapeDtypeStruct((width, frames), jnp.float32),
            jax.ShapeDtypeStruct((2, keys, width), jnp.bfloat16),
        ],
        compiler_params=pltpu.CompilerParams(vmem_limit_bytes=50 * 1024 * 1024),
        cost_estimate=pl.CostEstimate(
            flops=10 * frames * keys * width,
            bytes_accessed=8 * keys * width + 12 * frames * width,
            transcendentals=2 * pairs * frames * keys,
        ),
        name="attend_backward",
    )(length, query, grad, mixed, lse, joined, joined)


def with_halo(cells, sides, width):
    for axis, dim in sides:
        count = lax.axis_size(axis)
        ends = count - 1
        head = lax.slice_in_dim(cells, 0, width, axis=dim)
        tail = lax.slice_in_dim(cells, cells.shape[dim] - width, cells.shape[dim], axis=dim)
        cells = jnp.concatenate(
            [
                lax.ppermute(tail, axis, [(i, (i + 1) % count) for i in range(ends)]),
                cells,
                lax.ppermute(head, axis, [((i + 1) % count, i) for i in range(ends)]),
            ],
            axis=dim,
        )
    return cells


def layer_norm(values, gain):
    center = values - jnp.mean(values, -1, keepdims=True)
    spread = jnp.mean(center * center, -1, keepdims=True)
    return center * lax.rsqrt(spread + norm_eps) * gain


def rotary(values, position):
    half = values.shape[-1] // 2
    inverse = 10000.0 ** (-2.0 * jnp.arange(half, dtype=jnp.float32) / values.shape[-1])
    angle = position.astype(jnp.float32)[:, None] * inverse[None, :]
    cosine = jnp.cos(angle)[:, None, :]
    sine = jnp.sin(angle)[:, None, :]
    lower = values[..., :half]
    upper = values[..., half:]
    return jnp.concatenate([lower * cosine - upper * sine, lower * sine + upper * cosine], -1)


def swish(values):
    return values * jax.nn.sigmoid(values)


def tensor_total(partial_value):
    low = partial_value.astype(jnp.bfloat16)
    if lax.axis_size("tp") != 2:
        return lax.psum(low, "tp").astype(jnp.float32)
    other = lax.ppermute(low, "tp", [(0, 1), (1, 0)])
    return low.astype(jnp.float32) + other.astype(jnp.float32)


def group_sum_kernel(axes, sizes, x_ref, o_ref, slots, send_sem, recv_sem):
    places = [lax.axis_index(axis) for axis in axes]
    peers = []
    mine = 0
    for place, size in zip(places, sizes):
        mine = mine * size + place
    total = 1
    for size in sizes:
        total *= size
    for offset in range(1, total):
        rest, target = offset, {}
        for axis, place, size in reversed(list(zip(axes, places, sizes))):
            target[axis] = lax.rem(place + rest % size, size)
            rest //= size
        peers.append(target)
    barrier = pltpu.get_barrier_semaphore()
    for target in peers:
        pl.semaphore_signal(
            barrier, inc=1, device_id=target, device_id_type=pl.DeviceIdType.MESH
        )
    pl.semaphore_wait(barrier, total - 1)
    copies = []
    for number, target in enumerate(peers):
        copy = pltpu.make_async_remote_copy(
            src_ref=x_ref,
            dst_ref=slots.at[mine],
            send_sem=send_sem.at[number],
            recv_sem=recv_sem.at[number],
            device_id=target,
            device_id_type=pl.DeviceIdType.MESH,
        )
        copy.start()
        copies.append(copy)
    slots[mine] = x_ref[...]
    for copy in copies:
        copy.wait()
    result = slots[0]
    for number in range(1, total):
        result = result + slots[number]
    o_ref[...] = result


def group_sum(values, axes, number):
    sizes = [lax.axis_size(axis) for axis in axes]
    total = 1
    for size in sizes:
        total *= size
    return pl.pallas_call(
        functools.partial(group_sum_kernel, axes, sizes),
        out_shape=jax.ShapeDtypeStruct(values.shape, jnp.float32),
        in_specs=[pl.BlockSpec(memory_space=pltpu.VMEM)],
        out_specs=pl.BlockSpec(memory_space=pltpu.VMEM),
        scratch_shapes=[
            pltpu.VMEM((total,) + values.shape, jnp.float32),
            pltpu.SemaphoreType.DMA((total - 1,)),
            pltpu.SemaphoreType.DMA((total - 1,)),
        ],
        compiler_params=pltpu.CompilerParams(collective_id=number, has_side_effects=True),
        name="group_sum_" + str(number),
    )(values)


def flat_sum(arrays, stages):
    flat = jnp.concatenate([array.reshape(-1) for array in arrays])
    size = flat.shape[0]
    flat = jnp.pad(flat, (0, -size % 1024)).reshape(-1, 128)
    for axes, number in stages:
        flat = group_sum(flat, axes, number)
    flat = flat.reshape(-1)
    pieces, start = [], 0
    for array in arrays:
        pieces.append(lax.slice_in_dim(flat, start, start + array.size).reshape(array.shape))
        start += array.size
    return pieces


def gather_weights(*shards):
    rows = shards[0].shape[0]
    flat = jnp.concatenate([shard.reshape(rows, -1) for shard in shards], 1)
    part = rows // lax.axis_size("ctx")
    mine = lax.dynamic_slice_in_dim(flat, lax.axis_index("ctx") * part, part, 0)
    whole = lax.all_gather(mine, ("fsdp", "ctx"), axis=0, tiled=True)
    pieces, start = [], 0
    for shard in shards:
        width = shard.size // rows
        pieces.append(
            lax.slice_in_dim(whole, start, start + width, axis=1).reshape(-1, *shard.shape[1:])
        )
        start += width
    return pieces


def pack_grads(*grads):
    return jnp.concatenate(
        [grad.astype(jnp.bfloat16).reshape(grad.shape[0], -1) for grad in grads], 1
    )


def reduce_grads(packed, *shapes):
    part = lax.psum_scatter(packed, ("fsdp", "ctx"), scatter_dimension=0, tiled=True)
    whole = lax.all_gather(part, "ctx", axis=0, tiled=True)
    pieces, start = [], 0
    for shape in shapes:
        width = 1
        for size in shape[1:]:
            width *= size
        pieces.append(
            lax.slice_in_dim(whole, start, start + width, axis=1)
            .astype(jnp.float32)
            .reshape(-1, *shape[1:])
        )
        start += width
    return pieces


def attend_all(query_low, joined_all, lengths):
    batch, frames, heads, _ = query_low.shape
    if (heads * HEAD) % PAIR:
        return lax.map(attend_one, (query_low, joined_all, lengths))
    mixed, totals = [], []
    for row in range(batch):
        out, total = attend_forward(
            query_low[row].reshape(frames, -1), joined_all[row], lengths[row : row + 1]
        )
        mixed.append(out)
        totals.append(total)
    return (jnp.stack(mixed), jnp.stack(totals))


def attend_all_back(query_low, joined_all, lengths, log_total, mixed, mixed_grad):
    batch, frames, heads, _ = query_low.shape
    if (heads * HEAD) % PAIR:
        query_grad, joined_grad = lax.map(
            attend_back, (query_low, joined_all, lengths, log_total, mixed_grad)
        )
        width = heads * HEAD
        low = joined_grad.astype(jnp.bfloat16)
        return (query_grad, jnp.stack([low[..., :width], low[..., width:]], 1))
    queries, others = [], []
    for row in range(batch):
        query_grad, joined_grad = attend_backward(
            query_low[row].reshape(frames, -1),
            joined_all[row],
            lengths[row : row + 1],
            log_total[row],
            mixed[row],
            mixed_grad[row].reshape(frames, -1),
        )
        queries.append(query_grad.T.reshape(frames, heads, HEAD))
        others.append(joined_grad)
    return (jnp.stack(queries), jnp.stack(others))


def product_rows(left, right):
    return lax.dot_general(
        left, right, (((1,), (1,)), ((), ())), preferred_element_type=jnp.float32
    )


def product_cols(left, right):
    return lax.dot_general(
        left, right, (((0,), (0,)), ((), ())), preferred_element_type=jnp.float32
    )


def feed_forward(stream, gain, weight_up, weight_down):
    normed, norm_back = jax.vjp(layer_norm, stream, gain)
    normed_low = normed.astype(jnp.bfloat16)
    hidden = jnp.dot(normed_low, weight_up, preferred_element_type=jnp.float32)
    active, active_back = jax.vjp(swish, hidden)
    active_low = active.astype(jnp.bfloat16)
    branch = tensor_total(product_rows(active_low, weight_down))
    return (branch, (norm_back, normed_low, active_back, active_low))


def feed_backward(branch_grad, saved, weight_up, weight_down):
    norm_back, normed_low, active_back, active_low = saved
    grad_low = branch_grad.astype(jnp.bfloat16)
    down_grad = product_cols(grad_low, active_low)
    hidden_grad = active_back(jnp.dot(grad_low, weight_down, preferred_element_type=jnp.float32))[
        0
    ].astype(jnp.bfloat16)
    up_grad = product_cols(normed_low, hidden_grad)
    normed_grad = tensor_total(product_rows(hidden_grad, weight_up))
    stream_grad, gain_grad = norm_back(normed_grad)
    return (stream_grad, gain_grad, up_grad, down_grad)


def split_joined(joined, heads):
    width = heads * HEAD
    keys = joined[:, :width].reshape(joined.shape[0], heads, HEAD)
    values = joined[:, width:].reshape(joined.shape[0], heads, HEAD)
    return (keys, values)


def attend_scores(query, keys, length):
    scores = jnp.einsum("fhe,lhe->hfl", query, keys, preferred_element_type=jnp.float32)
    live_keys = jnp.arange(keys.shape[0]) < length
    return jnp.where(live_keys[None, None, :], scores, masked_score)


def attend_one(inputs):
    query, joined, length = inputs
    keys, values = split_joined(joined, query.shape[1])
    scores = attend_scores(query, keys, length)
    top = jnp.max(scores, -1, keepdims=True)
    raised = jnp.exp(scores - top)
    total = jnp.sum(raised, -1, keepdims=True)
    weights = (raised / total).astype(jnp.bfloat16)
    mixed = jnp.einsum("hfl,lhe->fhe", weights, values, preferred_element_type=jnp.float32)
    return (mixed.astype(jnp.bfloat16), (top + jnp.log(total))[..., 0])


def attend_back(inputs):
    query, joined, length, log_total, mixed_grad = inputs
    keys, values = split_joined(joined, query.shape[1])
    scores = attend_scores(query, keys, length)
    probs = jnp.exp(scores - log_total[..., None])
    probs_grad = jnp.einsum("fhe,lhe->hfl", mixed_grad, values, preferred_element_type=jnp.float32)
    center = jnp.sum(probs * probs_grad, -1, keepdims=True)
    score_grad = (probs * (probs_grad - center)).astype(jnp.bfloat16)
    query_grad = jnp.einsum("hfl,lhe->fhe", score_grad, keys, preferred_element_type=jnp.float32)
    keys_grad = jnp.einsum("hfl,fhe->lhe", score_grad, query, preferred_element_type=jnp.float32)
    values_grad = jnp.einsum(
        "hfl,fhe->lhe", probs.astype(jnp.bfloat16), mixed_grad, preferred_element_type=jnp.float32
    )
    frames_all = keys.shape[0]
    joined_grad = jnp.concatenate(
        [keys_grad.reshape(frames_all, -1), values_grad.reshape(frames_all, -1)], -1
    )
    return (query_grad, joined_grad)


def per_device(
    layer_input,
    out_grad,
    lengths,
    norm_gains,
    feed_up,
    feed_down,
    attend_in,
    attend_out,
    mixer_in,
    mixer_out,
    depth_kernel,
    batch_norm,
    final_up,
    final_down,
):
    batch, frames, width = layer_input.shape
    rows = batch * frames
    place = lax.axis_index("ctx") * frames + jnp.arange(frames, dtype=jnp.int32)
    live = (place[None, :] < lengths[:, None]).astype(jnp.float32)
    live_rows = live.reshape(rows, 1)
    live_cube = live[:, :, None]
    up_one, down_one = gather_weights(feed_up, feed_down)
    (proj_in,) = gather_weights(attend_in)
    proj_out, conv_in, conv_out = gather_weights(attend_out, mixer_in, mixer_out)
    stream = layer_input.reshape(rows, width)
    cotangent = out_grad.reshape(rows, width)
    branch_one, saved_one = feed_forward(stream, norm_gains[0], up_one, down_one)
    after_one = stream + 0.5 * branch_one
    normed, norm_back_two = jax.vjp(layer_norm, after_one, norm_gains[1])
    normed_two = normed.astype(jnp.bfloat16)
    projected = jnp.einsum("nd,dke->nke", normed_two, proj_in, preferred_element_type=jnp.float32)
    local_width = projected.shape[2]
    heads = local_width // HEAD
    split = projected.reshape(batch, frames, 3, heads, HEAD)

    def rotate_pair(query_raw, key_raw):
        return (rotary(query_raw, place) * HEAD ** (-0.5), rotary(key_raw, place))

    (query_rot, key_rot), rotate_back = jax.vjp(rotate_pair, split[:, :, 0], split[:, :, 1])
    query_low = query_rot.astype(jnp.bfloat16)
    joined = jnp.concatenate(
        [
            key_rot.astype(jnp.bfloat16).reshape(batch, frames, local_width),
            split[:, :, 2].astype(jnp.bfloat16).reshape(batch, frames, local_width),
        ],
        -1,
    )
    joined_all = lax.all_gather(joined, "ctx", axis=1, tiled=True)
    joined_all, late_up, late_down = lax.optimization_barrier((joined_all, final_up, final_down))
    up_two, down_two = gather_weights(late_up, late_down)
    mixed, log_total = attend_all(query_low, joined_all, lengths)
    if local_width % PAIR:
        mixed_rows = mixed.reshape(rows, local_width)
    else:
        mixed_rows = mixed.astype(jnp.bfloat16).transpose(0, 2, 1).reshape(rows, local_width)
    after_two = after_one + tensor_total(product_rows(mixed_rows, proj_out))
    normed, norm_back_three = jax.vjp(layer_norm, after_two, norm_gains[2])
    normed_three = normed.astype(jnp.bfloat16)
    gates = jnp.einsum("nd,dke->nke", normed_three, conv_in, preferred_element_type=jnp.float32)

    def gate_linear(values):
        return values[:, 0] * jax.nn.sigmoid(values[:, 1]) * live_rows

    gated, gate_back = jax.vjp(gate_linear, gates)
    channels = gated.shape[1]
    gated_low = gated.astype(jnp.bfloat16).reshape(batch, frames, channels)
    reach = KERNEL // 2
    padded = with_halo(gated_low, (("ctx", 1),), reach)
    filtered = jnp.zeros((batch, frames, channels), jnp.float32)
    for offset in range(KERNEL):
        filtered = filtered + depth_kernel[offset] * padded[:, offset : offset + frames].astype(
            jnp.float32
        )
    live_count = jnp.full((channels,), jnp.sum(live))
    sums = flat_sum(
        [
            jnp.sum(live_cube * filtered, (0, 1)),
            jnp.sum(live_cube * filtered * filtered, (0, 1)),
            live_count,
        ],
        [(("fsdp", "ctx"), 0)],
    )
    count = sums[2]
    mean = sums[0] / count
    variance = sums[1] / count - mean * mean
    rescale = lax.rsqrt(variance + norm_eps)
    unit = (filtered - mean) * rescale
    shifted = unit * batch_norm[0] + batch_norm[1]
    active, active_back = jax.vjp(swish, shifted.reshape(rows, channels))
    active_low = active.astype(jnp.bfloat16)
    after_three = after_two + tensor_total(product_rows(active_low, conv_out))
    branch_four, saved_four = feed_forward(after_three, norm_gains[3], up_two, down_two)
    after_four = after_three + 0.5 * branch_four
    result, final_back = jax.vjp(layer_norm, after_four, norm_gains[4])
    grad_four, gain_five = final_back(cotangent)
    stream_grad, gain_four, up_two_grad, down_two_grad = feed_backward(
        0.5 * grad_four, saved_four, up_two, down_two
    )
    grad_three = grad_four + stream_grad
    early, grad_three = lax.optimization_barrier(
        (pack_grads(up_two_grad, down_two_grad), grad_three)
    )
    up_two_grad, down_two_grad = reduce_grads(early, final_up.shape, final_down.shape)
    branch_low = grad_three.astype(jnp.bfloat16)
    conv_out_grad = product_cols(branch_low, active_low)
    shifted_grad = active_back(jnp.dot(branch_low, conv_out, preferred_element_type=jnp.float32))[
        0
    ].reshape(batch, frames, channels)
    bias_sum, scale_sum = flat_sum(
        [jnp.sum(shifted_grad, (0, 1)), jnp.sum(shifted_grad * unit, (0, 1))],
        [(("fsdp", "ctx"), 1)],
    )
    var_grad = -0.5 * rescale * rescale * batch_norm[0] * scale_sum
    first_grad = (-rescale * batch_norm[0] * bias_sum - 2.0 * mean * var_grad) / count
    second_grad = var_grad / count
    filtered_grad = (
        rescale * batch_norm[0] * shifted_grad
        + live_cube * (first_grad + 2.0 * filtered * second_grad)
    ).astype(jnp.bfloat16)
    padded_grad = with_halo(filtered_grad, (("ctx", 1),), reach)
    filtered_wide = filtered_grad.astype(jnp.float32)
    gated_grad = jnp.zeros((batch, frames, channels), jnp.float32)
    kernel_terms = []
    for offset in range(KERNEL):
        start = 2 * reach - offset
        gated_grad = gated_grad + depth_kernel[offset] * padded_grad[
            :, start : start + frames
        ].astype(jnp.float32)
        kernel_terms.append(
            jnp.sum(filtered_wide * padded[:, offset : offset + frames].astype(jnp.float32), (0, 1))
        )
    kernel_local = jnp.stack(kernel_terms)
    gates_grad = gate_back(gated_grad.reshape(rows, channels))[0].astype(jnp.bfloat16)
    conv_in_grad = jnp.einsum(
        "nd,nke->dke", normed_three, gates_grad, preferred_element_type=jnp.float32
    )
    normed_grad = tensor_total(
        jnp.einsum("nke,dke->nd", gates_grad, conv_in, preferred_element_type=jnp.float32)
    )
    stream_grad, gain_three = norm_back_three(normed_grad)
    grad_two = grad_three + stream_grad
    branch_low = grad_two.astype(jnp.bfloat16)
    proj_out_grad = product_cols(branch_low, mixed_rows)
    mixed_grad = (
        jnp.dot(branch_low, proj_out, preferred_element_type=jnp.float32)
        .astype(jnp.bfloat16)
        .reshape(batch, frames, heads, HEAD)
    )
    early = pack_grads(conv_in_grad, conv_out_grad, proj_out_grad)
    early, mixed_grad = lax.optimization_barrier((early, mixed_grad))
    conv_in_grad, conv_out_grad, proj_out_grad = reduce_grads(
        early, mixer_in.shape, mixer_out.shape, attend_out.shape
    )
    query_grad, joined_grad = attend_all_back(
        query_low, joined_all, lengths, log_total, mixed, mixed_grad
    )
    joined_local = lax.psum_scatter(
        joined_grad, "ctx", scatter_dimension=2, tiled=True
    ).astype(jnp.float32)
    key_grad = joined_local[:, 0].reshape(batch, frames, heads, HEAD)
    value_grad = joined_local[:, 1].reshape(batch, frames, heads, HEAD)
    query_raw_grad, key_raw_grad = rotate_back((query_grad, key_grad))
    proj_grad = (
        jnp.stack([query_raw_grad, key_raw_grad, value_grad], 2)
        .reshape(rows, 3, local_width)
        .astype(jnp.bfloat16)
    )
    proj_in_grad = jnp.einsum(
        "nd,nke->dke", normed_two, proj_grad, preferred_element_type=jnp.float32
    )
    normed_grad = tensor_total(
        jnp.einsum("nke,dke->nd", proj_grad, proj_in, preferred_element_type=jnp.float32)
    )
    stream_grad, gain_two = norm_back_two(normed_grad)
    grad_one = grad_two + stream_grad
    stream_grad, gain_one, up_one_grad, down_one_grad = feed_backward(
        0.5 * grad_one, saved_one, up_one, down_one
    )
    input_grad = grad_one + stream_grad
    gain_terms = jnp.stack([gain_one, gain_two, gain_three, gain_four, gain_five])
    gain_total, kernel_total = flat_sum(
        [gain_terms, kernel_local], [(("ctx",), 2), (("fsdp",), 3)]
    )
    up_one_grad, down_one_grad, proj_in_grad = reduce_grads(
        pack_grads(up_one_grad, down_one_grad, proj_in_grad),
        feed_up.shape,
        feed_down.shape,
        attend_in.shape,
    )
    return (
        result.reshape(batch, frames, width),
        input_grad.reshape(batch, frames, width),
        gain_total,
        up_one_grad,
        down_one_grad,
        proj_in_grad,
        proj_out_grad,
        conv_in_grad,
        conv_out_grad,
        kernel_total,
        jnp.stack([scale_sum, bias_sum]),
        up_two_grad,
        down_two_grad,
    )


def solution(mesh):
    placed = (
        P("fsdp", "ctx", None),
        P("fsdp", "ctx", None),
        P("fsdp"),
        P(),
        P("fsdp", "tp"),
        P("fsdp", "tp"),
        P("fsdp", None, "tp"),
        P("fsdp", "tp"),
        P("fsdp", None, "tp"),
        P("fsdp", "tp"),
        P(None, "tp"),
        P(None, "tp"),
        P("fsdp", "tp"),
        P("fsdp", "tp"),
    )
    return jax.shard_map(
        per_device,
        mesh=mesh,
        in_specs=placed,
        out_specs=(
            P("fsdp", "ctx", None),
            P("fsdp", "ctx", None),
            P(),
            P("fsdp", "tp"),
            P("fsdp", "tp"),
            P("fsdp", None, "tp"),
            P("fsdp", "tp"),
            P("fsdp", None, "tp"),
            P("fsdp", "tp"),
            P(None, "tp"),
            P(None, "tp"),
            P("fsdp", "tp"),
            P("fsdp", "tp"),
        ),
        check_vma=False,
    )
```

```python
import functools

import jax
import jax.numpy as jnp
from jax import lax
from jax.experimental import pallas as pl
from jax.experimental.pallas import tpu as pltpu
from jax.sharding import PartitionSpec as P

HEAD = 64
PAIR = 128
KERNEL = 31


norm_eps = 1e-05
masked_score = -1000000000.0


def split_heads(block, axis):
    spot = lax.broadcasted_iota(jnp.int32, block.shape, axis)
    zero = jnp.zeros_like(block)
    return (jnp.where(spot < HEAD, block, zero), jnp.where(spot < HEAD, zero, block))


def key_bias(meta_ref, chunk):
    start = meta_ref[1 + pl.program_id(0)]
    spot = start + lax.broadcasted_iota(jnp.int32, (chunk, 1), 0)
    return jnp.where(spot < meta_ref[0], 0.0, masked_score)


def attend_forward_kernel(meta_ref, q_ref, k_ref, v_ref, o_ref, lse_ref, qt_s, top_s, sum_s):
    chunk = k_ref.shape[0]
    step = pl.program_id(0)

    @pl.when(step == 0)
    def _():
        first, second = split_heads(q_ref[...].T, 0)
        qt_s[0] = first
        qt_s[1] = second
        top_s[...] = jnp.full_like(top_s, -jnp.inf)
        sum_s[...] = jnp.zeros_like(sum_s)
        o_ref[...] = jnp.zeros_like(o_ref)

    bias = key_bias(meta_ref, chunk)
    values = v_ref[...].T
    for j in range(2):
        scores = jnp.dot(k_ref[...], qt_s[j], preferred_element_type=jnp.float32) + bias
        old = top_s[j]
        top = jnp.maximum(old, jnp.max(scores, 0, keepdims=True))
        fade = jnp.exp(old - top)
        raised = jnp.exp(scores - top)
        top_s[j] = top
        sum_s[j] = sum_s[j] * fade + jnp.sum(raised, 0, keepdims=True)
        rows = slice(j * HEAD, (j + 1) * HEAD)
        o_ref[rows] = o_ref[rows] * fade + jnp.dot(
            values[rows], raised.astype(jnp.bfloat16), preferred_element_type=jnp.float32
        )

    @pl.when(step == pl.num_programs(0) - 1)
    def _():
        for j in range(2):
            rows = slice(j * HEAD, (j + 1) * HEAD)
            o_ref[rows] = o_ref[rows] / sum_s[j]
            lse_ref[j] = top_s[j] + jnp.log(sum_s[j])


def attend_forward(query, pair, joined, meta, chunk):
    frames = query.shape[0]
    keys = joined.shape[0]
    return pl.pallas_call(
        attend_forward_kernel,
        grid_spec=pltpu.PrefetchScalarGridSpec(
            num_scalar_prefetch=1,
            grid=(keys // chunk,),
            in_specs=[
                pl.BlockSpec((frames, PAIR), lambda c, n: (0, pair)),
                pl.BlockSpec((chunk, PAIR), lambda c, n: (c, 0)),
                pl.BlockSpec((chunk, PAIR), lambda c, n: (c, 1)),
            ],
            out_specs=[
                pl.BlockSpec((PAIR, frames), lambda c, n: (0, 0)),
                pl.BlockSpec((2, 1, frames), lambda c, n: (0, 0, 0)),
            ],
            scratch_shapes=[
                pltpu.VMEM((2, PAIR, frames), jnp.bfloat16),
                pltpu.VMEM((2, 1, frames), jnp.float32),
                pltpu.VMEM((2, 1, frames), jnp.float32),
            ],
        ),
        out_shape=[
            jax.ShapeDtypeStruct((PAIR, frames), jnp.float32),
            jax.ShapeDtypeStruct((2, 1, frames), jnp.float32),
        ],
        compiler_params=pltpu.CompilerParams(vmem_limit_bytes=50 * 1024 * 1024),
        cost_estimate=pl.CostEstimate(
            flops=4 * frames * keys * PAIR,
            bytes_accessed=4 * keys * PAIR + 6 * frames * PAIR,
            transcendentals=2 * frames * keys,
        ),
        name="attend_forward",
    )(meta, query, joined, joined)


def attend_backward_kernel(
    meta_ref, q_ref, g_ref, o_ref, lse_ref, k_ref, v_ref, dq_ref, dkv_ref,
    qt_s, gt_s, q_s, g_s, delta_s,
):
    chunk = k_ref.shape[0]

    @pl.when(pl.program_id(0) == 0)
    def _():
        query, grad = q_ref[...], g_ref[...]
        for j, part in enumerate(split_heads(query, 1)):
            q_s[j] = part
        for j, part in enumerate(split_heads(grad, 1)):
            g_s[j] = part
        grad_t = grad.T
        for j, part in enumerate(split_heads(query.T, 0)):
            qt_s[j] = part
        for j, part in enumerate(split_heads(grad_t, 0)):
            gt_s[j] = part
        product = grad_t.astype(jnp.float32) * o_ref[...]
        for j in range(2):
            delta_s[j] = jnp.sum(product[j * HEAD : (j + 1) * HEAD], 0, keepdims=True)
        dq_ref[...] = jnp.zeros_like(dq_ref)

    bias = key_bias(meta_ref, chunk)
    keys_t = k_ref[...].T
    dk = dv = None
    for j in range(2):
        scores = jnp.dot(k_ref[...], qt_s[j], preferred_element_type=jnp.float32) + bias
        probs = jnp.exp(scores - lse_ref[j])
        dp = jnp.dot(v_ref[...], gt_s[j], preferred_element_type=jnp.float32)
        ds = (probs * (dp - delta_s[j])).astype(jnp.bfloat16)
        dv_j = jnp.dot(probs.astype(jnp.bfloat16), g_s[j], preferred_element_type=jnp.float32)
        dk_j = jnp.dot(ds, q_s[j], preferred_element_type=jnp.float32)
        dk = dk_j if dk is None else dk + dk_j
        dv = dv_j if dv is None else dv + dv_j
        rows = slice(j * HEAD, (j + 1) * HEAD)
        dq_ref[rows] += jnp.dot(keys_t[rows], ds, preferred_element_type=jnp.float32)
    dkv_ref[:, :PAIR] = dk.astype(jnp.bfloat16)
    dkv_ref[:, PAIR:] = dv.astype(jnp.bfloat16)


def attend_backward(query, grad, pair, joined, meta, lse, mixed, chunk):
    frames = query.shape[0]
    keys = joined.shape[0]
    return pl.pallas_call(
        attend_backward_kernel,
        grid_spec=pltpu.PrefetchScalarGridSpec(
            num_scalar_prefetch=1,
            grid=(keys // chunk,),
            in_specs=[
                pl.BlockSpec((frames, PAIR), lambda c, n: (0, pair)),
                pl.BlockSpec((frames, PAIR), lambda c, n: (0, pair)),
                pl.BlockSpec((PAIR, frames), lambda c, n: (0, 0)),
                pl.BlockSpec((2, 1, frames), lambda c, n: (0, 0, 0)),
                pl.BlockSpec((chunk, PAIR), lambda c, n: (c, 0)),
                pl.BlockSpec((chunk, PAIR), lambda c, n: (c, 1)),
            ],
            out_specs=[
                pl.BlockSpec((PAIR, frames), lambda c, n: (0, 0)),
                pl.BlockSpec((chunk, 2 * PAIR), lambda c, n: (c, 0)),
            ],
            scratch_shapes=[
                pltpu.VMEM((2, PAIR, frames), jnp.bfloat16),
                pltpu.VMEM((2, PAIR, frames), jnp.bfloat16),
                pltpu.VMEM((2, frames, PAIR), jnp.bfloat16),
                pltpu.VMEM((2, frames, PAIR), jnp.bfloat16),
                pltpu.VMEM((2, 1, frames), jnp.float32),
            ],
        ),
        out_shape=[
            jax.ShapeDtypeStruct((PAIR, frames), jnp.float32),
            jax.ShapeDtypeStruct((keys, 2 * PAIR), jnp.bfloat16),
        ],
        compiler_params=pltpu.CompilerParams(vmem_limit_bytes=50 * 1024 * 1024),
        cost_estimate=pl.CostEstimate(
            flops=10 * frames * keys * PAIR,
            bytes_accessed=8 * keys * PAIR + 12 * frames * PAIR,
            transcendentals=2 * frames * keys,
        ),
        name="attend_backward",
    )(meta, query, grad, mixed, lse, joined, joined)


def with_halo(cells, sides, width):
    for axis, dim in sides:
        count = lax.axis_size(axis)
        ends = count - 1
        head = lax.slice_in_dim(cells, 0, width, axis=dim)
        tail = lax.slice_in_dim(cells, cells.shape[dim] - width, cells.shape[dim], axis=dim)
        cells = jnp.concatenate(
            [
                lax.ppermute(tail, axis, [(i, (i + 1) % count) for i in range(ends)]),
                cells,
                lax.ppermute(head, axis, [((i + 1) % count, i) for i in range(ends)]),
            ],
            axis=dim,
        )
    return cells


def layer_norm(values, gain):
    center = values - jnp.mean(values, -1, keepdims=True)
    spread = jnp.mean(center * center, -1, keepdims=True)
    return center * lax.rsqrt(spread + norm_eps) * gain


def rotary(values, position):
    half = values.shape[-1] // 2
    inverse = 10000.0 ** (-2.0 * jnp.arange(half, dtype=jnp.float32) / values.shape[-1])
    angle = position.astype(jnp.float32)[:, None] * inverse[None, :]
    cosine = jnp.cos(angle)[:, None, :]
    sine = jnp.sin(angle)[:, None, :]
    lower = values[..., :half]
    upper = values[..., half:]
    return jnp.concatenate([lower * cosine - upper * sine, lower * sine + upper * cosine], -1)


def swish(values):
    return values * jax.nn.sigmoid(values)


def tensor_total(partial_value):
    low = partial_value.astype(jnp.bfloat16)
    if lax.axis_size("tp") != 2:
        return lax.psum(low, "tp").astype(jnp.float32)
    other = lax.ppermute(low, "tp", [(0, 1), (1, 0)])
    return low.astype(jnp.float32) + other.astype(jnp.float32)


def group_sum_kernel(axes, sizes, x_ref, o_ref, slots, send_sem, recv_sem):
    places = [lax.axis_index(axis) for axis in axes]
    peers = []
    mine = 0
    for place, size in zip(places, sizes):
        mine = mine * size + place
    total = 1
    for size in sizes:
        total *= size
    for offset in range(1, total):
        rest, target = offset, {}
        for axis, place, size in reversed(list(zip(axes, places, sizes))):
            target[axis] = lax.rem(place + rest % size, size)
            rest //= size
        peers.append(target)
    barrier = pltpu.get_barrier_semaphore()
    for target in peers:
        pl.semaphore_signal(
            barrier, inc=1, device_id=target, device_id_type=pl.DeviceIdType.MESH
        )
    pl.semaphore_wait(barrier, total - 1)
    copies = []
    for number, target in enumerate(peers):
        copy = pltpu.make_async_remote_copy(
            src_ref=x_ref,
            dst_ref=slots.at[mine],
            send_sem=send_sem.at[number],
            recv_sem=recv_sem.at[number],
            device_id=target,
            device_id_type=pl.DeviceIdType.MESH,
        )
        copy.start()
        copies.append(copy)
    slots[mine] = x_ref[...]
    for copy in copies:
        copy.wait()
    result = slots[0]
    for number in range(1, total):
        result = result + slots[number]
    o_ref[...] = result


def group_sum(values, axes, number):
    sizes = [lax.axis_size(axis) for axis in axes]
    total = 1
    for size in sizes:
        total *= size
    return pl.pallas_call(
        functools.partial(group_sum_kernel, axes, sizes),
        out_shape=jax.ShapeDtypeStruct(values.shape, jnp.float32),
        in_specs=[pl.BlockSpec(memory_space=pltpu.VMEM)],
        out_specs=pl.BlockSpec(memory_space=pltpu.VMEM),
        scratch_shapes=[
            pltpu.VMEM((total,) + values.shape, jnp.float32),
            pltpu.SemaphoreType.DMA((total - 1,)),
            pltpu.SemaphoreType.DMA((total - 1,)),
        ],
        compiler_params=pltpu.CompilerParams(collective_id=number, has_side_effects=True),
        name="group_sum_" + str(number),
    )(values)


def flat_sum(arrays, stages):
    flat = jnp.concatenate([array.reshape(-1) for array in arrays])
    size = flat.shape[0]
    flat = jnp.pad(flat, (0, -size % 1024)).reshape(-1, 128)
    for axes, number in stages:
        flat = group_sum(flat, axes, number)
    flat = flat.reshape(-1)
    pieces, start = [], 0
    for array in arrays:
        pieces.append(lax.slice_in_dim(flat, start, start + array.size).reshape(array.shape))
        start += array.size
    return pieces


def gather_weights(*shards):
    rows = shards[0].shape[0]
    flat = jnp.concatenate([shard.reshape(rows, -1) for shard in shards], 1)
    part = rows // lax.axis_size("ctx")
    mine = lax.dynamic_slice_in_dim(flat, lax.axis_index("ctx") * part, part, 0)
    whole = lax.all_gather(mine, ("fsdp", "ctx"), axis=0, tiled=True)
    pieces, start = [], 0
    for shard in shards:
        width = shard.size // rows
        pieces.append(
            lax.slice_in_dim(whole, start, start + width, axis=1).reshape(-1, *shard.shape[1:])
        )
        start += width
    return pieces


def pack_grads(*grads):
    return jnp.concatenate(
        [grad.astype(jnp.bfloat16).reshape(grad.shape[0], -1) for grad in grads], 1
    )


def reduce_grads(packed, *shapes):
    part = lax.psum_scatter(packed, ("fsdp", "ctx"), scatter_dimension=0, tiled=True)
    whole = lax.all_gather(part, "ctx", axis=0, tiled=True)
    pieces, start = [], 0
    for shape in shapes:
        width = 1
        for size in shape[1:]:
            width *= size
        pieces.append(
            lax.slice_in_dim(whole, start, start + width, axis=1)
            .astype(jnp.float32)
            .reshape(-1, *shape[1:])
        )
        start += width
    return pieces


def swap(values, axis, bit):
    return lax.ppermute(values, axis, [(i, i ^ bit) for i in range(lax.axis_size(axis))])


def halve(values, axis, bit, dim):
    own = lax.axis_index(axis) // bit % 2
    keep = lax.dynamic_index_in_dim(values, own, dim, keepdims=False)
    send = lax.dynamic_index_in_dim(values, 1 - own, dim, keepdims=False)
    other = swap(send, axis, bit)
    return (keep.astype(jnp.float32) + other.astype(jnp.float32)).astype(jnp.bfloat16)


def double(values, axis, bit, dim):
    own = lax.axis_index(axis) // bit % 2
    other = swap(values, axis, bit)
    return jnp.where(
        own == 0, jnp.stack([values, other], dim), jnp.stack([other, values], dim)
    )


def reduce_by_swaps(grad):
    if lax.axis_size("fsdp") != 4 or lax.axis_size("ctx") != 4:
        return reduce_grads(pack_grads(grad), (grad.shape[0],) + grad.shape[1:])[0]
    low = grad.astype(jnp.bfloat16).reshape(grad.shape[0], -1)
    total = low.reshape(2, 2, 2, 2, -1, low.shape[1])
    total = halve(total, "ctx", 1, 3)
    total = halve(total, "ctx", 2, 2)
    total = halve(total, "fsdp", 1, 1)
    total = halve(total, "fsdp", 2, 0)
    total = double(total, "ctx", 2, 0)
    total = double(total, "ctx", 1, 1)
    return total.astype(jnp.float32).reshape(-1, *grad.shape[1:])


def attend_plan(lengths, frames, chunk):
    me = lax.axis_index("ctx")
    starts = [
        (me ^ block) * frames + start for block in (0, 2, 1, 3) for start in range(0, frames, chunk)
    ]
    return jnp.stack([lengths[0]] + starts).astype(jnp.int32)


def keys_everywhere(own):
    far = swap(own, "ctx", 2)
    near = swap(own, "ctx", 1)
    return jnp.concatenate([own, far, near, swap(far, "ctx", 1)], 0)


def keys_home(grads):
    half = grads.shape[0] // 2
    near = swap(grads[half:], "ctx", 1)
    both = grads[:half].astype(jnp.float32) + near.astype(jnp.float32)
    far = swap(both[half // 2 :].astype(jnp.bfloat16), "ctx", 2)
    return both[: half // 2] + far.astype(jnp.float32)


def product_rows(left, right):
    return lax.dot_general(
        left, right, (((1,), (1,)), ((), ())), preferred_element_type=jnp.float32
    )


def product_cols(left, right):
    return lax.dot_general(
        left, right, (((0,), (0,)), ((), ())), preferred_element_type=jnp.float32
    )


def feed_forward(stream, gain, weight_up, weight_down):
    normed, norm_back = jax.vjp(layer_norm, stream, gain)
    normed_low = normed.astype(jnp.bfloat16)
    hidden = jnp.dot(normed_low, weight_up, preferred_element_type=jnp.float32)
    active, active_back = jax.vjp(swish, hidden)
    active_low = active.astype(jnp.bfloat16)
    branch = tensor_total(product_rows(active_low, weight_down))
    return (branch, (norm_back, normed_low, active_back, active_low))


def feed_backward(branch_grad, saved, weight_up, weight_down):
    norm_back, normed_low, active_back, active_low = saved
    grad_low = branch_grad.astype(jnp.bfloat16)
    down_grad = product_cols(grad_low, active_low)
    hidden_grad = active_back(jnp.dot(grad_low, weight_down, preferred_element_type=jnp.float32))[
        0
    ].astype(jnp.bfloat16)
    up_grad = product_cols(normed_low, hidden_grad)
    normed_grad = tensor_total(product_rows(hidden_grad, weight_up))
    stream_grad, gain_grad = norm_back(normed_grad)
    return (stream_grad, gain_grad, up_grad, down_grad)


def split_joined(joined, heads):
    width = heads * HEAD
    keys = joined[:, :width].reshape(joined.shape[0], heads, HEAD)
    values = joined[:, width:].reshape(joined.shape[0], heads, HEAD)
    return (keys, values)


def attend_scores(query, keys, length):
    scores = jnp.einsum("fhe,lhe->hfl", query, keys, preferred_element_type=jnp.float32)
    live_keys = jnp.arange(keys.shape[0]) < length
    return jnp.where(live_keys[None, None, :], scores, masked_score)


def attend_one(inputs):
    query, joined, length = inputs
    keys, values = split_joined(joined, query.shape[1])
    scores = attend_scores(query, keys, length)
    top = jnp.max(scores, -1, keepdims=True)
    raised = jnp.exp(scores - top)
    total = jnp.sum(raised, -1, keepdims=True)
    weights = (raised / total).astype(jnp.bfloat16)
    mixed = jnp.einsum("hfl,lhe->fhe", weights, values, preferred_element_type=jnp.float32)
    return (mixed.astype(jnp.bfloat16), (top + jnp.log(total))[..., 0])


def attend_back(inputs):
    query, joined, length, log_total, mixed_grad = inputs
    keys, values = split_joined(joined, query.shape[1])
    scores = attend_scores(query, keys, length)
    probs = jnp.exp(scores - log_total[..., None])
    probs_grad = jnp.einsum("fhe,lhe->hfl", mixed_grad, values, preferred_element_type=jnp.float32)
    center = jnp.sum(probs * probs_grad, -1, keepdims=True)
    score_grad = (probs * (probs_grad - center)).astype(jnp.bfloat16)
    query_grad = jnp.einsum("hfl,lhe->fhe", score_grad, keys, preferred_element_type=jnp.float32)
    keys_grad = jnp.einsum("hfl,fhe->lhe", score_grad, query, preferred_element_type=jnp.float32)
    values_grad = jnp.einsum(
        "hfl,fhe->lhe", probs.astype(jnp.bfloat16), mixed_grad, preferred_element_type=jnp.float32
    )
    frames_all = keys.shape[0]
    joined_grad = jnp.concatenate(
        [keys_grad.reshape(frames_all, -1), values_grad.reshape(frames_all, -1)], -1
    )
    return (query_grad, joined_grad)


def per_device(
    layer_input,
    out_grad,
    lengths,
    norm_gains,
    feed_up,
    feed_down,
    attend_in,
    attend_out,
    mixer_in,
    mixer_out,
    depth_kernel,
    batch_norm,
    final_up,
    final_down,
):
    batch, frames, width = layer_input.shape
    rows = batch * frames
    place = lax.axis_index("ctx") * frames + jnp.arange(frames, dtype=jnp.int32)
    live = (place[None, :] < lengths[:, None]).astype(jnp.float32)
    live_rows = live.reshape(rows, 1)
    live_cube = live[:, :, None]
    up_one, down_one = gather_weights(feed_up, feed_down)
    (proj_in,) = gather_weights(attend_in)
    proj_out, conv_in, conv_out = gather_weights(attend_out, mixer_in, mixer_out)
    stream = layer_input.reshape(rows, width)
    cotangent = out_grad.reshape(rows, width)
    branch_one, saved_one = feed_forward(stream, norm_gains[0], up_one, down_one)
    after_one = stream + 0.5 * branch_one
    normed, norm_back_two = jax.vjp(layer_norm, after_one, norm_gains[1])
    normed_two = normed.astype(jnp.bfloat16)
    projected = jnp.einsum("nd,dke->nke", normed_two, proj_in, preferred_element_type=jnp.float32)
    local_width = projected.shape[2]
    heads = local_width // HEAD
    split = projected.reshape(batch, frames, 3, heads, HEAD)

    def rotate_pair(query_raw, key_raw):
        return (rotary(query_raw, place) * HEAD ** (-0.5), rotary(key_raw, place))

    (query_rot, key_rot), rotate_back = jax.vjp(rotate_pair, split[:, :, 0], split[:, :, 1])
    query_low = query_rot.astype(jnp.bfloat16)
    joined = jnp.concatenate(
        [
            key_rot.astype(jnp.bfloat16).reshape(batch, frames, local_width),
            split[:, :, 2].astype(jnp.bfloat16).reshape(batch, frames, local_width),
        ],
        -1,
    )
    paired = local_width % PAIR == 0 and batch == 1 and lax.axis_size("ctx") == 4
    pairs = local_width // PAIR
    chunk = min(frames, 512)
    if paired:
        plan = attend_plan(lengths, frames, chunk)
        query_rows = query_low.reshape(rows, local_width)
        pair_keys, pair_out, pair_lse = [], [], []
        for pair in range(pairs):
            own = [
                joined[0, :, side * local_width + pair * PAIR :][:, :PAIR] for side in range(2)
            ]
            pair_keys.append(keys_everywhere(jnp.concatenate(own, 1)))
        for pair in range(pairs):
            out, lse = attend_forward(query_rows, pair, pair_keys[pair], plan, chunk)
            pair_out.append(out)
            pair_lse.append(lse)
        mixed_rows = jnp.concatenate([out.astype(jnp.bfloat16).T for out in pair_out], 1)
    else:
        joined_all = lax.all_gather(joined, "ctx", axis=1, tiled=True)
        mixed, log_total = lax.map(attend_one, (query_low, joined_all, lengths))
        mixed_rows = mixed.reshape(rows, local_width)
    mixed_rows, late_up, late_down = lax.optimization_barrier((mixed_rows, final_up, final_down))
    up_two, down_two = gather_weights(late_up, late_down)
    after_two = after_one + tensor_total(product_rows(mixed_rows, proj_out))
    normed, norm_back_three = jax.vjp(layer_norm, after_two, norm_gains[2])
    normed_three = normed.astype(jnp.bfloat16)
    gates = jnp.einsum("nd,dke->nke", normed_three, conv_in, preferred_element_type=jnp.float32)

    def gate_linear(values):
        return values[:, 0] * jax.nn.sigmoid(values[:, 1]) * live_rows

    gated, gate_back = jax.vjp(gate_linear, gates)
    channels = gated.shape[1]
    gated_low = gated.astype(jnp.bfloat16).reshape(batch, frames, channels)
    reach = KERNEL // 2
    padded = with_halo(gated_low, (("ctx", 1),), reach)
    filtered = jnp.zeros((batch, frames, channels), jnp.float32)
    for offset in range(KERNEL):
        filtered = filtered + depth_kernel[offset] * padded[:, offset : offset + frames].astype(
            jnp.float32
        )
    live_count = jnp.full((channels,), jnp.sum(live))
    sums = flat_sum(
        [
            jnp.sum(live_cube * filtered, (0, 1)),
            jnp.sum(live_cube * filtered * filtered, (0, 1)),
            live_count,
        ],
        [(("fsdp", "ctx"), 0)],
    )
    count = sums[2]
    mean = sums[0] / count
    variance = sums[1] / count - mean * mean
    rescale = lax.rsqrt(variance + norm_eps)
    unit = (filtered - mean) * rescale
    shifted = unit * batch_norm[0] + batch_norm[1]
    active, active_back = jax.vjp(swish, shifted.reshape(rows, channels))
    active_low = active.astype(jnp.bfloat16)
    after_three = after_two + tensor_total(product_rows(active_low, conv_out))
    branch_four, saved_four = feed_forward(after_three, norm_gains[3], up_two, down_two)
    after_four = after_three + 0.5 * branch_four
    result, final_back = jax.vjp(layer_norm, after_four, norm_gains[4])
    grad_four, gain_five = final_back(cotangent)
    stream_grad, gain_four, up_two_grad, down_two_grad = feed_backward(
        0.5 * grad_four, saved_four, up_two, down_two
    )
    grad_three = grad_four + stream_grad
    early, grad_three = lax.optimization_barrier(
        (pack_grads(up_two_grad, down_two_grad), grad_three)
    )
    up_two_grad, down_two_grad = reduce_grads(early, final_up.shape, final_down.shape)
    branch_low = grad_three.astype(jnp.bfloat16)
    conv_out_grad = product_cols(branch_low, active_low)
    shifted_grad = active_back(jnp.dot(branch_low, conv_out, preferred_element_type=jnp.float32))[
        0
    ].reshape(batch, frames, channels)
    bias_sum, scale_sum = flat_sum(
        [jnp.sum(shifted_grad, (0, 1)), jnp.sum(shifted_grad * unit, (0, 1))],
        [(("fsdp", "ctx"), 1)],
    )
    var_grad = -0.5 * rescale * rescale * batch_norm[0] * scale_sum
    first_grad = (-rescale * batch_norm[0] * bias_sum - 2.0 * mean * var_grad) / count
    second_grad = var_grad / count
    filtered_grad = (
        rescale * batch_norm[0] * shifted_grad
        + live_cube * (first_grad + 2.0 * filtered * second_grad)
    ).astype(jnp.bfloat16)
    padded_grad = with_halo(filtered_grad, (("ctx", 1),), reach)
    filtered_wide = filtered_grad.astype(jnp.float32)
    gated_grad = jnp.zeros((batch, frames, channels), jnp.float32)
    kernel_terms = []
    for offset in range(KERNEL):
        start = 2 * reach - offset
        gated_grad = gated_grad + depth_kernel[offset] * padded_grad[
            :, start : start + frames
        ].astype(jnp.float32)
        kernel_terms.append(
            jnp.sum(filtered_wide * padded[:, offset : offset + frames].astype(jnp.float32), (0, 1))
        )
    kernel_local = jnp.stack(kernel_terms)
    gates_grad = gate_back(gated_grad.reshape(rows, channels))[0].astype(jnp.bfloat16)
    conv_in_grad = jnp.einsum(
        "nd,nke->dke", normed_three, gates_grad, preferred_element_type=jnp.float32
    )
    normed_grad = tensor_total(
        jnp.einsum("nke,dke->nd", gates_grad, conv_in, preferred_element_type=jnp.float32)
    )
    stream_grad, gain_three = norm_back_three(normed_grad)
    grad_two = grad_three + stream_grad
    branch_low = grad_two.astype(jnp.bfloat16)
    proj_out_grad = product_cols(branch_low, mixed_rows)
    mixed_grad = (
        jnp.dot(branch_low, proj_out, preferred_element_type=jnp.float32)
        .astype(jnp.bfloat16)
        .reshape(batch, frames, heads, HEAD)
    )
    early = pack_grads(conv_in_grad, conv_out_grad, proj_out_grad)
    early, mixed_grad = lax.optimization_barrier((early, mixed_grad))
    conv_in_grad, conv_out_grad, proj_out_grad = reduce_grads(
        early, mixer_in.shape, mixer_out.shape, attend_out.shape
    )
    if paired:
        grad_rows = mixed_grad.reshape(rows, local_width)
        home, queries = [], []
        for pair in range(pairs):
            query_part, keys_part = attend_backward(
                query_rows,
                grad_rows,
                pair,
                pair_keys[pair],
                plan,
                pair_lse[pair],
                pair_out[pair],
                chunk,
            )
            queries.append(query_part.T)
            home.append(keys_home(keys_part))
        query_grad = jnp.concatenate(queries, 1).reshape(batch, frames, heads, HEAD)
        key_grad, value_grad = (
            jnp.concatenate([part[:, side * PAIR :][:, :PAIR] for part in home], 1).reshape(
                batch, frames, heads, HEAD
            )
            for side in range(2)
        )
    else:
        query_grad, joined_grad = lax.map(
            attend_back, (query_low, joined_all, lengths, log_total, mixed_grad)
        )
        joined_local = lax.psum_scatter(
            joined_grad.astype(jnp.bfloat16), "ctx", scatter_dimension=1, tiled=True
        ).astype(jnp.float32)
        key_grad = joined_local[..., :local_width].reshape(batch, frames, heads, HEAD)
        value_grad = joined_local[..., local_width:].reshape(batch, frames, heads, HEAD)
    query_raw_grad, key_raw_grad = rotate_back((query_grad, key_grad))
    proj_grad = (
        jnp.stack([query_raw_grad, key_raw_grad, value_grad], 2)
        .reshape(rows, 3, local_width)
        .astype(jnp.bfloat16)
    )
    proj_in_grad = jnp.einsum(
        "nd,nke->dke", normed_two, proj_grad, preferred_element_type=jnp.float32
    )
    normed_grad = tensor_total(
        jnp.einsum("nke,dke->nd", proj_grad, proj_in, preferred_element_type=jnp.float32)
    )
    stream_grad, gain_two = norm_back_two(normed_grad)
    grad_one = grad_two + stream_grad
    stream_grad, gain_one, up_one_grad, down_one_grad = feed_backward(
        0.5 * grad_one, saved_one, up_one, down_one
    )
    input_grad = grad_one + stream_grad
    gain_terms = jnp.stack([gain_one, gain_two, gain_three, gain_four, gain_five])
    gain_total, kernel_total = flat_sum(
        [gain_terms, kernel_local], [(("ctx",), 2), (("fsdp",), 3)]
    )
    proj_in_grad = reduce_by_swaps(proj_in_grad)
    down_one_grad = reduce_by_swaps(down_one_grad)
    up_one_grad = reduce_by_swaps(up_one_grad)
    return (
        result.reshape(batch, frames, width),
        input_grad.reshape(batch, frames, width),
        gain_total,
        up_one_grad,
        down_one_grad,
        proj_in_grad,
        proj_out_grad,
        conv_in_grad,
        conv_out_grad,
        kernel_total,
        jnp.stack([scale_sum, bias_sum]),
        up_two_grad,
        down_two_grad,
    )


def solution(mesh):
    placed = (
        P("fsdp", "ctx", None),
        P("fsdp", "ctx", None),
        P("fsdp"),
        P(),
        P("fsdp", "tp"),
        P("fsdp", "tp"),
        P("fsdp", None, "tp"),
        P("fsdp", "tp"),
        P("fsdp", None, "tp"),
        P("fsdp", "tp"),
        P(None, "tp"),
        P(None, "tp"),
        P("fsdp", "tp"),
        P("fsdp", "tp"),
    )
    return jax.shard_map(
        per_device,
        mesh=mesh,
        in_specs=placed,
        out_specs=(
            P("fsdp", "ctx", None),
            P("fsdp", "ctx", None),
            P(),
            P("fsdp", "tp"),
            P("fsdp", "tp"),
            P("fsdp", None, "tp"),
            P("fsdp", "tp"),
            P("fsdp", None, "tp"),
            P("fsdp", "tp"),
            P(None, "tp"),
            P(None, "tp"),
            P("fsdp", "tp"),
            P("fsdp", "tp"),
        ),
        check_vma=False,
    )
```

```python
import functools

import jax
import jax.numpy as jnp
from jax import lax
from jax.experimental import pallas as pl
from jax.experimental.pallas import tpu as pltpu
from jax.sharding import PartitionSpec as P

HEAD = 64
PAIR = 128
KERNEL = 31


norm_eps = 1e-05
masked_score = -1000000000.0


def split_heads(block, axis):
    spot = lax.broadcasted_iota(jnp.int32, block.shape, axis)
    zero = jnp.zeros_like(block)
    return (jnp.where(spot < HEAD, block, zero), jnp.where(spot < HEAD, zero, block))


def key_bias(meta_ref, chunk):
    start = meta_ref[1 + pl.program_id(0)]
    spot = start + lax.broadcasted_iota(jnp.int32, (chunk, 1), 0)
    return jnp.where(spot < meta_ref[0], 0.0, masked_score)


def attend_forward_kernel(last, meta_ref, q_ref, k_ref, v_ref, *refs):
    if last:
        o_in, top_in, sum_in, o_ref, lse_ref, qt_s, top_s, sum_s = refs
    else:
        o_ref, top_s, sum_s, qt_s = refs
    chunk = k_ref.shape[0]
    step = pl.program_id(0)

    @pl.when(step == 0)
    def _():
        first, second = split_heads(q_ref[...].T, 0)
        qt_s[0] = first
        qt_s[1] = second
        if last:
            top_s[...] = top_in[...]
            sum_s[...] = sum_in[...]
            o_ref[...] = o_in[...]
        else:
            top_s[...] = jnp.full_like(top_s, -jnp.inf)
            sum_s[...] = jnp.zeros_like(sum_s)
            o_ref[...] = jnp.zeros_like(o_ref)

    bias = key_bias(meta_ref, chunk)
    values = v_ref[...].T
    for j in range(2):
        scores = jnp.dot(k_ref[...], qt_s[j], preferred_element_type=jnp.float32) + bias
        old = top_s[j]
        top = jnp.maximum(old, jnp.max(scores, 0, keepdims=True))
        fade = jnp.exp(old - top)
        raised = jnp.exp(scores - top)
        top_s[j] = top
        sum_s[j] = sum_s[j] * fade + jnp.sum(raised, 0, keepdims=True)
        rows = slice(j * HEAD, (j + 1) * HEAD)
        o_ref[rows] = o_ref[rows] * fade + jnp.dot(
            values[rows], raised.astype(jnp.bfloat16), preferred_element_type=jnp.float32
        )

    if last:

        @pl.when(step == pl.num_programs(0) - 1)
        def _():
            for j in range(2):
                rows = slice(j * HEAD, (j + 1) * HEAD)
                o_ref[rows] = o_ref[rows] / sum_s[j]
                lse_ref[j] = top_s[j] + jnp.log(sum_s[j])


def attend_forward(query, pair, joined, meta, chunk, state):
    frames = query.shape[0]
    keys = joined.shape[0]
    last = len(state) > 0
    wide = pl.BlockSpec((PAIR, frames), lambda c, n: (0, 0))
    row = pl.BlockSpec((2, 1, frames), lambda c, n: (0, 0, 0))
    row_scratch = pltpu.VMEM((2, 1, frames), jnp.float32)
    row_shape = jax.ShapeDtypeStruct((2, 1, frames), jnp.float32)
    return pl.pallas_call(
        functools.partial(attend_forward_kernel, last),
        grid_spec=pltpu.PrefetchScalarGridSpec(
            num_scalar_prefetch=1,
            grid=(keys // chunk,),
            in_specs=[
                pl.BlockSpec((frames, PAIR), lambda c, n: (0, pair)),
                pl.BlockSpec((chunk, PAIR), lambda c, n: (c, 0)),
                pl.BlockSpec((chunk, PAIR), lambda c, n: (c, 1)),
            ]
            + ([wide, row, row] if last else []),
            out_specs=[wide, row] if last else [wide, row, row],
            scratch_shapes=[pltpu.VMEM((2, PAIR, frames), jnp.bfloat16)]
            + ([row_scratch, row_scratch] if last else []),
        ),
        out_shape=[jax.ShapeDtypeStruct((PAIR, frames), jnp.float32), row_shape]
        + ([] if last else [row_shape]),
        compiler_params=pltpu.CompilerParams(vmem_limit_bytes=50 * 1024 * 1024),
        cost_estimate=pl.CostEstimate(
            flops=16 * frames * keys * PAIR,
            bytes_accessed=4 * keys * PAIR + 6 * frames * PAIR,
            transcendentals=2 * frames * keys,
        ),
        name="attend_forward",
    )(meta, query, joined, joined, *state)


def attend_backward_kernel(
    meta_ref, q_ref, g_ref, o_ref, lse_ref, k_ref, v_ref, dq_ref, dkv_ref,
    qt_s, gt_s, q_s, g_s, delta_s,
):
    chunk = k_ref.shape[0]

    @pl.when(pl.program_id(0) == 0)
    def _():
        query, grad = q_ref[...], g_ref[...]
        for j, part in enumerate(split_heads(query, 1)):
            q_s[j] = part
        for j, part in enumerate(split_heads(grad, 1)):
            g_s[j] = part
        grad_t = grad.T
        for j, part in enumerate(split_heads(query.T, 0)):
            qt_s[j] = part
        for j, part in enumerate(split_heads(grad_t, 0)):
            gt_s[j] = part
        product = grad_t.astype(jnp.float32) * o_ref[...]
        for j in range(2):
            delta_s[j] = jnp.sum(product[j * HEAD : (j + 1) * HEAD], 0, keepdims=True)
        dq_ref[...] = jnp.zeros_like(dq_ref)

    bias = key_bias(meta_ref, chunk)
    keys_t = k_ref[...].T
    dk = dv = None
    for j in range(2):
        scores = jnp.dot(k_ref[...], qt_s[j], preferred_element_type=jnp.float32) + bias
        probs = jnp.exp(scores - lse_ref[j])
        dp = jnp.dot(v_ref[...], gt_s[j], preferred_element_type=jnp.float32)
        ds = (probs * (dp - delta_s[j])).astype(jnp.bfloat16)
        dv_j = jnp.dot(probs.astype(jnp.bfloat16), g_s[j], preferred_element_type=jnp.float32)
        dk_j = jnp.dot(ds, q_s[j], preferred_element_type=jnp.float32)
        dk = dk_j if dk is None else dk + dk_j
        dv = dv_j if dv is None else dv + dv_j
        rows = slice(j * HEAD, (j + 1) * HEAD)
        dq_ref[rows] += jnp.dot(keys_t[rows], ds, preferred_element_type=jnp.float32)
    dkv_ref[:, :PAIR] = dk.astype(jnp.bfloat16)
    dkv_ref[:, PAIR:] = dv.astype(jnp.bfloat16)


def attend_backward(query, grad, pair, joined, meta, lse, mixed, chunk):
    frames = query.shape[0]
    keys = joined.shape[0]
    return pl.pallas_call(
        attend_backward_kernel,
        grid_spec=pltpu.PrefetchScalarGridSpec(
            num_scalar_prefetch=1,
            grid=(keys // chunk,),
            in_specs=[
                pl.BlockSpec((frames, PAIR), lambda c, n: (0, pair)),
                pl.BlockSpec((frames, PAIR), lambda c, n: (0, pair)),
                pl.BlockSpec((PAIR, frames), lambda c, n: (0, 0)),
                pl.BlockSpec((2, 1, frames), lambda c, n: (0, 0, 0)),
                pl.BlockSpec((chunk, PAIR), lambda c, n: (c, 0)),
                pl.BlockSpec((chunk, PAIR), lambda c, n: (c, 1)),
            ],
            out_specs=[
                pl.BlockSpec((PAIR, frames), lambda c, n: (0, 0)),
                pl.BlockSpec((chunk, 2 * PAIR), lambda c, n: (c, 0)),
            ],
            scratch_shapes=[
                pltpu.VMEM((2, PAIR, frames), jnp.bfloat16),
                pltpu.VMEM((2, PAIR, frames), jnp.bfloat16),
                pltpu.VMEM((2, frames, PAIR), jnp.bfloat16),
                pltpu.VMEM((2, frames, PAIR), jnp.bfloat16),
                pltpu.VMEM((2, 1, frames), jnp.float32),
            ],
        ),
        out_shape=[
            jax.ShapeDtypeStruct((PAIR, frames), jnp.float32),
            jax.ShapeDtypeStruct((keys, 2 * PAIR), jnp.bfloat16),
        ],
        compiler_params=pltpu.CompilerParams(vmem_limit_bytes=50 * 1024 * 1024),
        cost_estimate=pl.CostEstimate(
            flops=30 * frames * keys * PAIR,
            bytes_accessed=8 * keys * PAIR + 12 * frames * PAIR,
            transcendentals=2 * frames * keys,
        ),
        name="attend_backward",
    )(meta, query, grad, mixed, lse, joined, joined)


def with_halo(cells, sides, width):
    for axis, dim in sides:
        count = lax.axis_size(axis)
        ends = count - 1
        head = lax.slice_in_dim(cells, 0, width, axis=dim)
        tail = lax.slice_in_dim(cells, cells.shape[dim] - width, cells.shape[dim], axis=dim)
        cells = jnp.concatenate(
            [
                lax.ppermute(tail, axis, [(i, (i + 1) % count) for i in range(ends)]),
                cells,
                lax.ppermute(head, axis, [((i + 1) % count, i) for i in range(ends)]),
            ],
            axis=dim,
        )
    return cells


def layer_norm(values, gain):
    center = values - jnp.mean(values, -1, keepdims=True)
    spread = jnp.mean(center * center, -1, keepdims=True)
    return center * lax.rsqrt(spread + norm_eps) * gain


def rotary(values, position):
    half = values.shape[-1] // 2
    inverse = 10000.0 ** (-2.0 * jnp.arange(half, dtype=jnp.float32) / values.shape[-1])
    angle = position.astype(jnp.float32)[:, None] * inverse[None, :]
    cosine = jnp.cos(angle)[:, None, :]
    sine = jnp.sin(angle)[:, None, :]
    lower = values[..., :half]
    upper = values[..., half:]
    return jnp.concatenate([lower * cosine - upper * sine, lower * sine + upper * cosine], -1)


def swish(values):
    return values * jax.nn.sigmoid(values)


def tensor_total(partial_value):
    low = partial_value.astype(jnp.bfloat16)
    if lax.axis_size("tp") != 2:
        return lax.psum(low, "tp").astype(jnp.float32)
    other = lax.ppermute(low, "tp", [(0, 1), (1, 0)])
    return low.astype(jnp.float32) + other.astype(jnp.float32)


def group_sum_kernel(axes, sizes, x_ref, o_ref, slots, send_sem, recv_sem):
    places = [lax.axis_index(axis) for axis in axes]
    peers = []
    mine = 0
    for place, size in zip(places, sizes):
        mine = mine * size + place
    total = 1
    for size in sizes:
        total *= size
    for offset in range(1, total):
        rest, target = offset, {}
        for axis, place, size in reversed(list(zip(axes, places, sizes))):
            target[axis] = lax.rem(place + rest % size, size)
            rest //= size
        peers.append(target)
    barrier = pltpu.get_barrier_semaphore()
    for target in peers:
        pl.semaphore_signal(
            barrier, inc=1, device_id=target, device_id_type=pl.DeviceIdType.MESH
        )
    pl.semaphore_wait(barrier, total - 1)
    copies = []
    for number, target in enumerate(peers):
        copy = pltpu.make_async_remote_copy(
            src_ref=x_ref,
            dst_ref=slots.at[mine],
            send_sem=send_sem.at[number],
            recv_sem=recv_sem.at[number],
            device_id=target,
            device_id_type=pl.DeviceIdType.MESH,
        )
        copy.start()
        copies.append(copy)
    slots[mine] = x_ref[...]
    for copy in copies:
        copy.wait()
    result = slots[0]
    for number in range(1, total):
        result = result + slots[number]
    o_ref[...] = result


def group_sum(values, axes, number):
    sizes = [lax.axis_size(axis) for axis in axes]
    total = 1
    for size in sizes:
        total *= size
    return pl.pallas_call(
        functools.partial(group_sum_kernel, axes, sizes),
        out_shape=jax.ShapeDtypeStruct(values.shape, jnp.float32),
        in_specs=[pl.BlockSpec(memory_space=pltpu.VMEM)],
        out_specs=pl.BlockSpec(memory_space=pltpu.VMEM),
        scratch_shapes=[
            pltpu.VMEM((total,) + values.shape, jnp.float32),
            pltpu.SemaphoreType.DMA((total - 1,)),
            pltpu.SemaphoreType.DMA((total - 1,)),
        ],
        compiler_params=pltpu.CompilerParams(collective_id=number, has_side_effects=True),
        name="group_sum_" + str(number),
    )(values)


def flat_sum(arrays, stages):
    flat = jnp.concatenate([array.reshape(-1) for array in arrays])
    size = flat.shape[0]
    flat = jnp.pad(flat, (0, -size % 1024)).reshape(-1, 128)
    for axes, number in stages:
        flat = group_sum(flat, axes, number)
    flat = flat.reshape(-1)
    pieces, start = [], 0
    for array in arrays:
        pieces.append(lax.slice_in_dim(flat, start, start + array.size).reshape(array.shape))
        start += array.size
    return pieces


def gather_weights(*shards):
    rows = shards[0].shape[0]
    flat = jnp.concatenate([shard.reshape(rows, -1) for shard in shards], 1)
    part = rows // lax.axis_size("ctx")
    mine = lax.dynamic_slice_in_dim(flat, lax.axis_index("ctx") * part, part, 0)
    whole = lax.all_gather(mine, ("fsdp", "ctx"), axis=0, tiled=True)
    pieces, start = [], 0
    for shard in shards:
        width = shard.size // rows
        pieces.append(
            lax.slice_in_dim(whole, start, start + width, axis=1).reshape(-1, *shard.shape[1:])
        )
        start += width
    return pieces


def pack_grads(*grads):
    return jnp.concatenate(
        [grad.astype(jnp.bfloat16).reshape(grad.shape[0], -1) for grad in grads], 1
    )


def reduce_grads(packed, *shapes):
    part = lax.psum_scatter(packed, ("fsdp", "ctx"), scatter_dimension=0, tiled=True)
    if lax.axis_size("ctx") == 4:
        whole = double(double(part, "ctx", 2, 0), "ctx", 1, 1).reshape(-1, part.shape[1])
    else:
        whole = lax.all_gather(part, "ctx", axis=0, tiled=True)
    pieces, start = [], 0
    for shape in shapes:
        width = 1
        for size in shape[1:]:
            width *= size
        pieces.append(
            lax.slice_in_dim(whole, start, start + width, axis=1)
            .astype(jnp.float32)
            .reshape(-1, *shape[1:])
        )
        start += width
    return pieces


def swap(values, axis, bit):
    return lax.ppermute(values, axis, [(i, i ^ bit) for i in range(lax.axis_size(axis))])


def halve(values, axis, bit, dim):
    own = lax.axis_index(axis) // bit % 2
    keep = lax.dynamic_index_in_dim(values, own, dim, keepdims=False)
    send = lax.dynamic_index_in_dim(values, 1 - own, dim, keepdims=False)
    other = swap(send, axis, bit)
    return (keep.astype(jnp.float32) + other.astype(jnp.float32)).astype(jnp.bfloat16)


def double(values, axis, bit, dim):
    own = lax.axis_index(axis) // bit % 2
    other = swap(values, axis, bit)
    return jnp.where(
        own == 0, jnp.stack([values, other], dim), jnp.stack([other, values], dim)
    )


def reduce_by_swaps(grad):
    if lax.axis_size("fsdp") != 4 or lax.axis_size("ctx") != 4:
        return reduce_grads(pack_grads(grad), (grad.shape[0],) + grad.shape[1:])[0]
    low = grad.astype(jnp.bfloat16).reshape(grad.shape[0], -1)
    total = low.reshape(2, 2, 2, 2, -1, low.shape[1])
    total = halve(total, "ctx", 1, 3)
    total = halve(total, "ctx", 2, 2)
    total = halve(total, "fsdp", 1, 1)
    total = halve(total, "fsdp", 2, 0)
    total = double(total, "ctx", 2, 0)
    total = double(total, "ctx", 1, 1)
    return total.astype(jnp.float32).reshape(-1, *grad.shape[1:])


def attend_plans(lengths, frames, chunk):
    me = lax.axis_index("ctx")
    return [
        jnp.stack(
            [lengths[0]]
            + [
                (me ^ block) * frames + start
                for block in blocks
                for start in range(0, frames, chunk)
            ]
        ).astype(jnp.int32)
        for blocks in ((0, 1), (2, 3))
    ]


def sum_by_swaps(arrays, axes):
    flat = jnp.concatenate([array.reshape(-1) for array in arrays])
    size = flat.shape[0]
    flat = jnp.pad(flat, (0, -size % 1024)).reshape(-1, 128)
    for axis in axes:
        bit = 1
        while bit < lax.axis_size(axis):
            flat = flat + swap(flat, axis, bit)
            bit *= 2
    flat = flat.reshape(-1)
    pieces, start = [], 0
    for array in arrays:
        pieces.append(lax.slice_in_dim(flat, start, start + array.size).reshape(array.shape))
        start += array.size
    return pieces


def product_rows(left, right):
    return lax.dot_general(
        left, right, (((1,), (1,)), ((), ())), preferred_element_type=jnp.float32
    )


def product_cols(left, right):
    return lax.dot_general(
        left, right, (((0,), (0,)), ((), ())), preferred_element_type=jnp.float32
    )


def feed_forward(stream, gain, weight_up, weight_down):
    normed, norm_back = jax.vjp(layer_norm, stream, gain)
    normed_low = normed.astype(jnp.bfloat16)
    hidden = jnp.dot(normed_low, weight_up, preferred_element_type=jnp.float32)
    active, active_back = jax.vjp(swish, hidden)
    active_low = active.astype(jnp.bfloat16)
    branch = tensor_total(product_rows(active_low, weight_down))
    return (branch, (norm_back, normed_low, active_back, active_low))


def feed_backward(branch_grad, saved, weight_up, weight_down, gain_early):
    norm_back, normed_low, active_back, active_low = saved
    grad_low = branch_grad.astype(jnp.bfloat16)
    down_grad = product_cols(grad_low, active_low)
    hidden_grad = active_back(jnp.dot(grad_low, weight_down, preferred_element_type=jnp.float32))[
        0
    ].astype(jnp.bfloat16)
    up_grad = product_cols(normed_low, hidden_grad)
    normed_part = product_rows(hidden_grad, weight_up)
    _, gain_part = norm_back(normed_part)
    normed_low_grad = normed_part.astype(jnp.bfloat16)
    if gain_early:
        gain_part, normed_low_grad = lax.optimization_barrier((gain_part, normed_low_grad))
    stream_grad, _ = norm_back(tensor_total(normed_low_grad))
    return (stream_grad, gain_part, up_grad, down_grad)


def split_joined(joined, heads):
    width = heads * HEAD
    keys = joined[:, :width].reshape(joined.shape[0], heads, HEAD)
    values = joined[:, width:].reshape(joined.shape[0], heads, HEAD)
    return (keys, values)


def attend_scores(query, keys, length):
    scores = jnp.einsum("fhe,lhe->hfl", query, keys, preferred_element_type=jnp.float32)
    live_keys = jnp.arange(keys.shape[0]) < length
    return jnp.where(live_keys[None, None, :], scores, masked_score)


def attend_one(inputs):
    query, joined, length = inputs
    keys, values = split_joined(joined, query.shape[1])
    scores = attend_scores(query, keys, length)
    top = jnp.max(scores, -1, keepdims=True)
    raised = jnp.exp(scores - top)
    total = jnp.sum(raised, -1, keepdims=True)
    weights = (raised / total).astype(jnp.bfloat16)
    mixed = jnp.einsum("hfl,lhe->fhe", weights, values, preferred_element_type=jnp.float32)
    return (mixed.astype(jnp.bfloat16), (top + jnp.log(total))[..., 0])


def attend_back(inputs):
    query, joined, length, log_total, mixed_grad = inputs
    keys, values = split_joined(joined, query.shape[1])
    scores = attend_scores(query, keys, length)
    probs = jnp.exp(scores - log_total[..., None])
    probs_grad = jnp.einsum("fhe,lhe->hfl", mixed_grad, values, preferred_element_type=jnp.float32)
    center = jnp.sum(probs * probs_grad, -1, keepdims=True)
    score_grad = (probs * (probs_grad - center)).astype(jnp.bfloat16)
    query_grad = jnp.einsum("hfl,lhe->fhe", score_grad, keys, preferred_element_type=jnp.float32)
    keys_grad = jnp.einsum("hfl,fhe->lhe", score_grad, query, preferred_element_type=jnp.float32)
    values_grad = jnp.einsum(
        "hfl,fhe->lhe", probs.astype(jnp.bfloat16), mixed_grad, preferred_element_type=jnp.float32
    )
    frames_all = keys.shape[0]
    joined_grad = jnp.concatenate(
        [keys_grad.reshape(frames_all, -1), values_grad.reshape(frames_all, -1)], -1
    )
    return (query_grad, joined_grad)


def per_device(
    layer_input,
    out_grad,
    lengths,
    norm_gains,
    feed_up,
    feed_down,
    attend_in,
    attend_out,
    mixer_in,
    mixer_out,
    depth_kernel,
    batch_norm,
    final_up,
    final_down,
):
    batch, frames, width = layer_input.shape
    rows = batch * frames
    place = lax.axis_index("ctx") * frames + jnp.arange(frames, dtype=jnp.int32)
    live = (place[None, :] < lengths[:, None]).astype(jnp.float32)
    live_rows = live.reshape(rows, 1)
    live_cube = live[:, :, None]
    up_one, down_one = gather_weights(feed_up, feed_down)
    (proj_in,) = gather_weights(attend_in)
    proj_out, conv_in, conv_out = gather_weights(attend_out, mixer_in, mixer_out)
    stream = layer_input.reshape(rows, width)
    cotangent = out_grad.reshape(rows, width)
    branch_one, saved_one = feed_forward(stream, norm_gains[0], up_one, down_one)
    after_one = stream + 0.5 * branch_one
    normed, norm_back_two = jax.vjp(layer_norm, after_one, norm_gains[1])
    normed_two = normed.astype(jnp.bfloat16)
    projected = jnp.einsum("nd,dke->nke", normed_two, proj_in, preferred_element_type=jnp.float32)
    local_width = projected.shape[2]
    heads = local_width // HEAD
    split = projected.reshape(batch, frames, 3, heads, HEAD)

    def rotate_pair(query_raw, key_raw):
        return (rotary(query_raw, place) * HEAD ** (-0.5), rotary(key_raw, place))

    (query_rot, key_rot), rotate_back = jax.vjp(rotate_pair, split[:, :, 0], split[:, :, 1])
    query_low = query_rot.astype(jnp.bfloat16)
    joined = jnp.concatenate(
        [
            key_rot.astype(jnp.bfloat16).reshape(batch, frames, local_width),
            split[:, :, 2].astype(jnp.bfloat16).reshape(batch, frames, local_width),
        ],
        -1,
    )
    paired = local_width % PAIR == 0 and batch == 1 and lax.axis_size("ctx") == 4
    pairs = local_width // PAIR
    chunk = min(frames, 512)
    if paired:
        near_plan, far_plan = attend_plans(lengths, frames, chunk)
        query_rows = query_low.reshape(rows, local_width)
        owns = [
            jnp.concatenate(
                [joined[0, :, side * local_width + pair * PAIR :][:, :PAIR] for side in range(2)],
                1,
            )
            for pair in range(pairs)
        ]
        cores = [swap(own, "ctx", 1) for own in owns]
        chips = [swap(own, "ctx", 2) for own in owns]
        near_keys = [jnp.concatenate([own, core], 0) for own, core in zip(owns, cores)]
        far_keys, states, pair_out, pair_lse = [], [], [], []
        for pair in range(pairs):
            state = attend_forward(query_rows, pair, near_keys[pair], near_plan, chunk, ())
            near_plan, far_plan, chip, *state = lax.optimization_barrier(
                (near_plan, far_plan, chips[pair], *state)
            )
            states.append(state)
            far_keys.append(jnp.concatenate([chip, swap(chip, "ctx", 1)], 0))
        for pair in range(pairs):
            out, lse = attend_forward(
                query_rows, pair, far_keys[pair], far_plan, chunk, tuple(states[pair])
            )
            near_plan, far_plan, out, lse = lax.optimization_barrier(
                (near_plan, far_plan, out, lse)
            )
            pair_out.append(out)
            pair_lse.append(lse)
        mixed_rows = jnp.concatenate([out.astype(jnp.bfloat16).T for out in pair_out], 1)
    else:
        joined_all = lax.all_gather(joined, "ctx", axis=1, tiled=True)
        mixed, log_total = lax.map(attend_one, (query_low, joined_all, lengths))
        mixed_rows = mixed.reshape(rows, local_width)
    mixed_rows, late_up, late_down = lax.optimization_barrier((mixed_rows, final_up, final_down))
    up_two, down_two = gather_weights(late_up, late_down)
    after_two = after_one + tensor_total(product_rows(mixed_rows, proj_out))
    normed, norm_back_three = jax.vjp(layer_norm, after_two, norm_gains[2])
    normed_three = normed.astype(jnp.bfloat16)
    gates = jnp.einsum("nd,dke->nke", normed_three, conv_in, preferred_element_type=jnp.float32)

    def gate_linear(values):
        return values[:, 0] * jax.nn.sigmoid(values[:, 1]) * live_rows

    gated, gate_back = jax.vjp(gate_linear, gates)
    channels = gated.shape[1]
    gated_low = gated.astype(jnp.bfloat16).reshape(batch, frames, channels)
    reach = KERNEL // 2
    padded = with_halo(gated_low, (("ctx", 1),), reach)
    filtered = jnp.zeros((batch, frames, channels), jnp.float32)
    for offset in range(KERNEL):
        filtered = filtered + depth_kernel[offset] * padded[:, offset : offset + frames].astype(
            jnp.float32
        )
    live_count = jnp.full((channels,), jnp.sum(live))
    sums = flat_sum(
        [
            jnp.sum(live_cube * filtered, (0, 1)),
            jnp.sum(live_cube * filtered * filtered, (0, 1)),
            live_count,
        ],
        [(("fsdp", "ctx"), 0)],
    )
    count = sums[2]
    mean = sums[0] / count
    variance = sums[1] / count - mean * mean
    rescale = lax.rsqrt(variance + norm_eps)
    unit = (filtered - mean) * rescale
    shifted = unit * batch_norm[0] + batch_norm[1]
    active, active_back = jax.vjp(swish, shifted.reshape(rows, channels))
    active_low = active.astype(jnp.bfloat16)
    after_three = after_two + tensor_total(product_rows(active_low, conv_out))
    branch_four, saved_four = feed_forward(after_three, norm_gains[3], up_two, down_two)
    after_four = after_three + 0.5 * branch_four
    result, final_back = jax.vjp(layer_norm, after_four, norm_gains[4])
    grad_four, gain_five = final_back(cotangent)
    stream_grad, gain_four, up_two_grad, down_two_grad = feed_backward(
        0.5 * grad_four, saved_four, up_two, down_two, False
    )
    grad_three = grad_four + stream_grad
    early, grad_three = lax.optimization_barrier(
        (pack_grads(up_two_grad, down_two_grad), grad_three)
    )
    up_two_grad, down_two_grad = reduce_grads(early, final_up.shape, final_down.shape)
    branch_low = grad_three.astype(jnp.bfloat16)
    conv_out_grad = product_cols(branch_low, active_low)
    shifted_grad = active_back(jnp.dot(branch_low, conv_out, preferred_element_type=jnp.float32))[
        0
    ].reshape(batch, frames, channels)
    bias_sum, scale_sum = flat_sum(
        [jnp.sum(shifted_grad, (0, 1)), jnp.sum(shifted_grad * unit, (0, 1))],
        [(("fsdp", "ctx"), 1)],
    )
    var_grad = -0.5 * rescale * rescale * batch_norm[0] * scale_sum
    first_grad = (-rescale * batch_norm[0] * bias_sum - 2.0 * mean * var_grad) / count
    second_grad = var_grad / count
    filtered_grad = (
        rescale * batch_norm[0] * shifted_grad
        + live_cube * (first_grad + 2.0 * filtered * second_grad)
    ).astype(jnp.bfloat16)
    padded_grad = with_halo(filtered_grad, (("ctx", 1),), reach)
    filtered_wide = filtered_grad.astype(jnp.float32)
    gated_grad = jnp.zeros((batch, frames, channels), jnp.float32)
    kernel_terms = []
    for offset in range(KERNEL):
        start = 2 * reach - offset
        gated_grad = gated_grad + depth_kernel[offset] * padded_grad[
            :, start : start + frames
        ].astype(jnp.float32)
        kernel_terms.append(
            jnp.sum(filtered_wide * padded[:, offset : offset + frames].astype(jnp.float32), (0, 1))
        )
    kernel_local = jnp.stack(kernel_terms)
    gates_grad = gate_back(gated_grad.reshape(rows, channels))[0].astype(jnp.bfloat16)
    (kernel_total,) = sum_by_swaps([kernel_local], ("ctx", "fsdp"))
    conv_in_grad = jnp.einsum(
        "nd,nke->dke", normed_three, gates_grad, preferred_element_type=jnp.float32
    )
    normed_grad = tensor_total(
        jnp.einsum("nke,dke->nd", gates_grad, conv_in, preferred_element_type=jnp.float32)
    )
    stream_grad, gain_three = norm_back_three(normed_grad)
    share = 1.0 / lax.axis_size("tp")
    gain_three, gain_four, gain_five = sum_by_swaps(
        [gain_three * share, gain_four, gain_five * share], ("ctx", "fsdp", "tp")
    )
    grad_two = grad_three + stream_grad
    branch_low = grad_two.astype(jnp.bfloat16)
    proj_out_grad = product_cols(branch_low, mixed_rows)
    mixed_grad = (
        jnp.dot(branch_low, proj_out, preferred_element_type=jnp.float32)
        .astype(jnp.bfloat16)
        .reshape(batch, frames, heads, HEAD)
    )
    early = pack_grads(conv_in_grad, conv_out_grad, proj_out_grad)
    early, mixed_grad = lax.optimization_barrier((early, mixed_grad))
    conv_in_grad, conv_out_grad, proj_out_grad = reduce_grads(
        early, mixer_in.shape, mixer_out.shape, attend_out.shape
    )
    if paired:
        grad_rows = mixed_grad.reshape(rows, local_width)
        half = frames
        far_grads, far_parts, home, queries = [], [], [], []
        for pair in range(pairs):
            query_far, keys_far = attend_backward(
                query_rows, grad_rows, pair, far_keys[pair], far_plan,
                pair_lse[pair], pair_out[pair], chunk,
            )
            near_plan, far_plan, query_far, keys_far = lax.optimization_barrier(
                (near_plan, far_plan, query_far, keys_far)
            )
            queries.append(query_far)
            far_grads.append((keys_far[:half], swap(keys_far[half:], "ctx", 1)))
        for pair in range(pairs):
            one, other = far_grads[pair]
            part = (one.astype(jnp.float32) + other.astype(jnp.float32)).astype(jnp.bfloat16)
            near_plan, part = lax.optimization_barrier((near_plan, part))
            far_parts.append(swap(part, "ctx", 2))
            query_near, keys_near = attend_backward(
                query_rows, grad_rows, pair, near_keys[pair], near_plan,
                pair_lse[pair], pair_out[pair], chunk,
            )
            near_plan, query_near, keys_near = lax.optimization_barrier(
                (near_plan, query_near, keys_near)
            )
            queries[pair] = (queries[pair] + query_near).T
            home.append((keys_near[:half], swap(keys_near[half:], "ctx", 1)))
        home = [
            one.astype(jnp.float32) + other.astype(jnp.float32) + far.astype(jnp.float32)
            for (one, other), far in zip(home, far_parts)
        ]
        query_grad = jnp.concatenate(queries, 1).reshape(batch, frames, heads, HEAD)
        key_grad, value_grad = (
            jnp.concatenate([part[:, side * PAIR :][:, :PAIR] for part in home], 1).reshape(
                batch, frames, heads, HEAD
            )
            for side in range(2)
        )
    else:
        query_grad, joined_grad = lax.map(
            attend_back, (query_low, joined_all, lengths, log_total, mixed_grad)
        )
        joined_local = lax.psum_scatter(
            joined_grad.astype(jnp.bfloat16), "ctx", scatter_dimension=1, tiled=True
        ).astype(jnp.float32)
        key_grad = joined_local[..., :local_width].reshape(batch, frames, heads, HEAD)
        value_grad = joined_local[..., local_width:].reshape(batch, frames, heads, HEAD)
    query_raw_grad, key_raw_grad = rotate_back((query_grad, key_grad))
    proj_grad = (
        jnp.stack([query_raw_grad, key_raw_grad, value_grad], 2)
        .reshape(rows, 3, local_width)
        .astype(jnp.bfloat16)
    )
    normed_part = jnp.einsum(
        "nke,dke->nd", proj_grad, proj_in, preferred_element_type=jnp.float32
    ).astype(jnp.bfloat16)
    normed_part, proj_late = lax.optimization_barrier((normed_part, proj_grad))
    proj_in_grad = jnp.einsum(
        "nd,nke->dke", normed_two, proj_late, preferred_element_type=jnp.float32
    )
    normed_grad = tensor_total(normed_part)
    stream_grad, gain_two = norm_back_two(normed_grad)
    grad_one = grad_two + stream_grad
    stream_grad, gain_one, up_one_grad, down_one_grad = feed_backward(
        0.5 * grad_one, saved_one, up_one, down_one, True
    )
    input_grad = grad_one + stream_grad
    share = 1.0 / lax.axis_size("tp")
    gain_one, gain_two = sum_by_swaps([gain_one, gain_two * share], ("ctx", "fsdp", "tp"))
    gain_total = jnp.stack([gain_one, gain_two, gain_three, gain_four, gain_five])
    proj_in_grad = reduce_by_swaps(proj_in_grad)
    down_one_grad = reduce_by_swaps(down_one_grad)
    up_one_grad = reduce_by_swaps(up_one_grad)
    return (
        result.reshape(batch, frames, width),
        input_grad.reshape(batch, frames, width),
        gain_total,
        up_one_grad,
        down_one_grad,
        proj_in_grad,
        proj_out_grad,
        conv_in_grad,
        conv_out_grad,
        kernel_total,
        jnp.stack([scale_sum, bias_sum]),
        up_two_grad,
        down_two_grad,
    )


def solution(mesh):
    placed = (
        P("fsdp", "ctx", None),
        P("fsdp", "ctx", None),
        P("fsdp"),
        P(),
        P("fsdp", "tp"),
        P("fsdp", "tp"),
        P("fsdp", None, "tp"),
        P("fsdp", "tp"),
        P("fsdp", None, "tp"),
        P("fsdp", "tp"),
        P(None, "tp"),
        P(None, "tp"),
        P("fsdp", "tp"),
        P("fsdp", "tp"),
    )
    return jax.shard_map(
        per_device,
        mesh=mesh,
        in_specs=placed,
        out_specs=(
            P("fsdp", "ctx", None),
            P("fsdp", "ctx", None),
            P(),
            P("fsdp", "tp"),
            P("fsdp", "tp"),
            P("fsdp", None, "tp"),
            P("fsdp", "tp"),
            P("fsdp", None, "tp"),
            P("fsdp", "tp"),
            P(None, "tp"),
            P(None, "tp"),
            P("fsdp", "tp"),
            P("fsdp", "tp"),
        ),
        check_vma=False,
    )
```

```python
import functools

import jax
import jax.numpy as jnp
from jax import lax
from jax.experimental import pallas as pl
from jax.experimental.pallas import tpu as pltpu
from jax.sharding import PartitionSpec as P

HEAD = 64
PAIR = 128
KERNEL = 31


norm_eps = 1e-05
masked_score = -1000000000.0


def split_heads(block, axis):
    spot = lax.broadcasted_iota(jnp.int32, block.shape, axis)
    zero = jnp.zeros_like(block)
    return (jnp.where(spot < HEAD, block, zero), jnp.where(spot < HEAD, zero, block))


def key_bias(meta_ref, chunk):
    start = meta_ref[1 + pl.program_id(0)]
    spot = start + lax.broadcasted_iota(jnp.int32, (chunk, 1), 0)
    return jnp.where(spot < meta_ref[0], 0.0, masked_score)


def attend_forward_kernel(last, meta_ref, q_ref, k_ref, v_ref, *refs):
    if last:
        o_in, top_in, sum_in, o_ref, lse_ref, qt_s, top_s, sum_s = refs
    else:
        o_ref, top_s, sum_s, qt_s = refs
    chunk = k_ref.shape[0]
    step = pl.program_id(0)

    @pl.when(step == 0)
    def _():
        first, second = split_heads(q_ref[...].T, 0)
        qt_s[0] = first
        qt_s[1] = second
        if last:
            top_s[...] = top_in[...]
            sum_s[...] = sum_in[...]
            o_ref[...] = o_in[...]
        else:
            top_s[...] = jnp.full_like(top_s, -jnp.inf)
            sum_s[...] = jnp.zeros_like(sum_s)
            o_ref[...] = jnp.zeros_like(o_ref)

    bias = key_bias(meta_ref, chunk)
    values = v_ref[...].T
    for j in range(2):
        scores = jnp.dot(k_ref[...], qt_s[j], preferred_element_type=jnp.float32) + bias
        old = top_s[j]
        top = jnp.maximum(old, jnp.max(scores, 0, keepdims=True))
        fade = jnp.exp(old - top)
        raised = jnp.exp(scores - top)
        top_s[j] = top
        sum_s[j] = sum_s[j] * fade + jnp.sum(raised, 0, keepdims=True)
        rows = slice(j * HEAD, (j + 1) * HEAD)
        o_ref[rows] = o_ref[rows] * fade + jnp.dot(
            values[rows], raised.astype(jnp.bfloat16), preferred_element_type=jnp.float32
        )

    if last:

        @pl.when(step == pl.num_programs(0) - 1)
        def _():
            for j in range(2):
                rows = slice(j * HEAD, (j + 1) * HEAD)
                o_ref[rows] = o_ref[rows] / sum_s[j]
                lse_ref[j] = top_s[j] + jnp.log(sum_s[j])


def attend_forward(query, pair, joined, meta, chunk, state):
    frames = query.shape[0]
    keys = joined.shape[0]
    last = len(state) > 0
    wide = pl.BlockSpec((PAIR, frames), lambda c, n: (0, 0))
    row = pl.BlockSpec((2, 1, frames), lambda c, n: (0, 0, 0))
    row_scratch = pltpu.VMEM((2, 1, frames), jnp.float32)
    row_shape = jax.ShapeDtypeStruct((2, 1, frames), jnp.float32)
    return pl.pallas_call(
        functools.partial(attend_forward_kernel, last),
        grid_spec=pltpu.PrefetchScalarGridSpec(
            num_scalar_prefetch=1,
            grid=(keys // chunk,),
            in_specs=[
                pl.BlockSpec((frames, PAIR), lambda c, n: (0, pair)),
                pl.BlockSpec((chunk, PAIR), lambda c, n: (c, 0)),
                pl.BlockSpec((chunk, PAIR), lambda c, n: (c, 1)),
            ]
            + ([wide, row, row] if last else []),
            out_specs=[wide, row] if last else [wide, row, row],
            scratch_shapes=[pltpu.VMEM((2, PAIR, frames), jnp.bfloat16)]
            + ([row_scratch, row_scratch] if last else []),
        ),
        out_shape=[jax.ShapeDtypeStruct((PAIR, frames), jnp.float32), row_shape]
        + ([] if last else [row_shape]),
        compiler_params=pltpu.CompilerParams(vmem_limit_bytes=50 * 1024 * 1024),
        cost_estimate=pl.CostEstimate(
            flops=16 * frames * keys * PAIR,
            bytes_accessed=4 * keys * PAIR + 6 * frames * PAIR,
            transcendentals=2 * frames * keys,
        ),
        name="attend_forward",
    )(meta, query, joined, joined, *state)


def attend_backward_kernel(
    meta_ref, q_ref, g_ref, o_ref, lse_ref, k_ref, v_ref, dq_ref, dkv_ref,
    qt_s, gt_s, q_s, g_s, delta_s,
):
    chunk = k_ref.shape[0]

    @pl.when(pl.program_id(0) == 0)
    def _():
        query, grad = q_ref[...], g_ref[...]
        for j, part in enumerate(split_heads(query, 1)):
            q_s[j] = part
        for j, part in enumerate(split_heads(grad, 1)):
            g_s[j] = part
        grad_t = grad.T
        for j, part in enumerate(split_heads(query.T, 0)):
            qt_s[j] = part
        for j, part in enumerate(split_heads(grad_t, 0)):
            gt_s[j] = part
        product = grad_t.astype(jnp.float32) * o_ref[...]
        for j in range(2):
            delta_s[j] = jnp.sum(product[j * HEAD : (j + 1) * HEAD], 0, keepdims=True)
        dq_ref[...] = jnp.zeros_like(dq_ref)

    bias = key_bias(meta_ref, chunk)
    keys_t = k_ref[...].T
    dk = dv = None
    for j in range(2):
        scores = jnp.dot(k_ref[...], qt_s[j], preferred_element_type=jnp.float32) + bias
        probs = jnp.exp(scores - lse_ref[j])
        dp = jnp.dot(v_ref[...], gt_s[j], preferred_element_type=jnp.float32)
        ds = (probs * (dp - delta_s[j])).astype(jnp.bfloat16)
        dv_j = jnp.dot(probs.astype(jnp.bfloat16), g_s[j], preferred_element_type=jnp.float32)
        dk_j = jnp.dot(ds, q_s[j], preferred_element_type=jnp.float32)
        dk = dk_j if dk is None else dk + dk_j
        dv = dv_j if dv is None else dv + dv_j
        rows = slice(j * HEAD, (j + 1) * HEAD)
        dq_ref[rows] += jnp.dot(keys_t[rows], ds, preferred_element_type=jnp.float32)
    dkv_ref[:, :PAIR] = dk.astype(jnp.bfloat16)
    dkv_ref[:, PAIR:] = dv.astype(jnp.bfloat16)


def attend_backward(query, grad, pair, joined, meta, lse, mixed, chunk):
    frames = query.shape[0]
    keys = joined.shape[0]
    return pl.pallas_call(
        attend_backward_kernel,
        grid_spec=pltpu.PrefetchScalarGridSpec(
            num_scalar_prefetch=1,
            grid=(keys // chunk,),
            in_specs=[
                pl.BlockSpec((frames, PAIR), lambda c, n: (0, pair)),
                pl.BlockSpec((frames, PAIR), lambda c, n: (0, pair)),
                pl.BlockSpec((PAIR, frames), lambda c, n: (0, 0)),
                pl.BlockSpec((2, 1, frames), lambda c, n: (0, 0, 0)),
                pl.BlockSpec((chunk, PAIR), lambda c, n: (c, 0)),
                pl.BlockSpec((chunk, PAIR), lambda c, n: (c, 1)),
            ],
            out_specs=[
                pl.BlockSpec((PAIR, frames), lambda c, n: (0, 0)),
                pl.BlockSpec((chunk, 2 * PAIR), lambda c, n: (c, 0)),
            ],
            scratch_shapes=[
                pltpu.VMEM((2, PAIR, frames), jnp.bfloat16),
                pltpu.VMEM((2, PAIR, frames), jnp.bfloat16),
                pltpu.VMEM((2, frames, PAIR), jnp.bfloat16),
                pltpu.VMEM((2, frames, PAIR), jnp.bfloat16),
                pltpu.VMEM((2, 1, frames), jnp.float32),
            ],
        ),
        out_shape=[
            jax.ShapeDtypeStruct((PAIR, frames), jnp.float32),
            jax.ShapeDtypeStruct((keys, 2 * PAIR), jnp.bfloat16),
        ],
        compiler_params=pltpu.CompilerParams(vmem_limit_bytes=50 * 1024 * 1024),
        cost_estimate=pl.CostEstimate(
            flops=30 * frames * keys * PAIR,
            bytes_accessed=8 * keys * PAIR + 12 * frames * PAIR,
            transcendentals=2 * frames * keys,
        ),
        name="attend_backward",
    )(meta, query, grad, mixed, lse, joined, joined)


def with_halo(cells, sides, width):
    for axis, dim in sides:
        count = lax.axis_size(axis)
        ends = count - 1
        head = lax.slice_in_dim(cells, 0, width, axis=dim)
        tail = lax.slice_in_dim(cells, cells.shape[dim] - width, cells.shape[dim], axis=dim)
        cells = jnp.concatenate(
            [
                lax.ppermute(tail, axis, [(i, (i + 1) % count) for i in range(ends)]),
                cells,
                lax.ppermute(head, axis, [((i + 1) % count, i) for i in range(ends)]),
            ],
            axis=dim,
        )
    return cells


def halo_parts(cells, width):
    count = lax.axis_size("ctx")
    left = lax.ppermute(cells[-width:], "ctx", [(i, i + 1) for i in range(count - 1)])
    right = lax.ppermute(cells[:width], "ctx", [(i + 1, i) for i in range(count - 1)])
    return (left, cells, right)


def layer_norm(values, gain):
    center = values - jnp.mean(values, -1, keepdims=True)
    spread = jnp.mean(center * center, -1, keepdims=True)
    return center * lax.rsqrt(spread + norm_eps) * gain


def rotary(values, position):
    half = values.shape[-1] // 2
    inverse = 10000.0 ** (-2.0 * jnp.arange(half, dtype=jnp.float32) / values.shape[-1])
    angle = position.astype(jnp.float32)[:, None] * inverse[None, :]
    cosine = jnp.cos(angle)[:, None, :]
    sine = jnp.sin(angle)[:, None, :]
    lower = values[..., :half]
    upper = values[..., half:]
    return jnp.concatenate([lower * cosine - upper * sine, lower * sine + upper * cosine], -1)


def swish(values):
    return values * jax.nn.sigmoid(values)


def tensor_total(partial_value):
    low = partial_value.astype(jnp.bfloat16)
    if lax.axis_size("tp") != 2:
        return lax.psum(low, "tp").astype(jnp.float32)
    other = lax.ppermute(low, "tp", [(0, 1), (1, 0)])
    return low.astype(jnp.float32) + other.astype(jnp.float32)


def fill_wide(wide, left_ref, body_ref, right_ref):
    frames, reach = body_ref.shape[0], left_ref.shape[0]
    wide[1 : 1 + reach] = left_ref[...].astype(jnp.float32)
    wide[1 + reach : 1 + reach + frames] = body_ref[...].astype(jnp.float32)
    wide[1 + reach + frames : 1 + 2 * reach + frames] = right_ref[...].astype(jnp.float32)


def conv_forward_kernel(
    live_ref, left_ref, body_ref, right_ref, weight_ref, o_ref, sums_ref, wide
):
    frames, channels = o_ref.shape
    block = 64
    fill_wide(wide, left_ref, body_ref, right_ref)
    sums_ref[...] = jnp.zeros_like(sums_ref)

    @pl.loop(0, frames // block)
    def _(step):
        row = pl.multiple_of(step * block, block)
        spot = row + lax.broadcasted_iota(jnp.int32, (block, 1), 0)
        live = (spot < live_ref[0]).astype(jnp.float32)
        for lane in range(0, channels, PAIR):
            lanes = slice(lane, lane + PAIR)
            total = jnp.zeros((block, PAIR), jnp.float32)
            near = wide[pl.ds(row, block + 32), lanes]
            for tap in range(KERNEL):
                total = total + weight_ref[tap : tap + 1, lanes] * near[tap + 1 : tap + 1 + block]
            o_ref[pl.ds(row, block), lanes] = total
            kept = live * total
            sums_ref[0:8, lanes] += jnp.sum(kept.reshape(block // 8, 8, PAIR), 0)
            sums_ref[8:16, lanes] += jnp.sum((kept * total).reshape(block // 8, 8, PAIR), 0)


def conv_forward(parts, weight, live_frames):
    frames, channels = parts[1].shape
    out, sums = pl.pallas_call(
        conv_forward_kernel,
        out_shape=[
            jax.ShapeDtypeStruct((frames, channels), jnp.float32),
            jax.ShapeDtypeStruct((16, channels), jnp.float32),
        ],
        in_specs=[
            pl.BlockSpec(memory_space=pltpu.SMEM),
        ]
        + [pl.BlockSpec(memory_space=pltpu.VMEM)] * 4,
        out_specs=[pl.BlockSpec(memory_space=pltpu.VMEM)] * 2,
        scratch_shapes=[pltpu.VMEM((frames + 32, channels), jnp.float32)],
        cost_estimate=pl.CostEstimate(
            flops=2 * KERNEL * frames * channels,
            bytes_accessed=6 * frames * channels,
            transcendentals=0,
        ),
        name="conv_forward",
    )(live_frames, *parts, weight)
    sums = jnp.sum(sums.reshape(2, 8, channels), 1)
    return (out, sums[0], sums[1])


def conv_backward_kernel(
    left_ref, body_ref, right_ref, left_grad, body_grad, right_grad, weight_ref,
    o_ref, taps_ref, wide, grads,
):
    frames, channels = o_ref.shape
    block = 64
    reach = KERNEL // 2
    fill_wide(wide, left_ref, body_ref, right_ref)
    fill_wide(grads, left_grad, body_grad, right_grad)
    taps_ref[...] = jnp.zeros_like(taps_ref)

    @pl.loop(0, frames // block)
    def _(step):
        row = pl.multiple_of(step * block, block)
        for lane in range(0, channels, PAIR):
            lanes = slice(lane, lane + PAIR)
            total = jnp.zeros((block, PAIR), jnp.float32)
            near = grads[pl.ds(row, block + 32), lanes]
            for tap in range(KERNEL):
                start = 2 * reach - tap
                total = total + weight_ref[tap : tap + 1, lanes] * near[start + 1 : start + 1 + block]
            o_ref[pl.ds(row, block), lanes] = total
            own = near[reach + 1 : reach + 1 + block]
            value = wide[pl.ds(row, block + 32), lanes]
            for tap in range(KERNEL):
                product = own * value[tap + 1 : tap + 1 + block]
                taps_ref[8 * tap : 8 * tap + 8, lanes] += jnp.sum(
                    product.reshape(block // 8, 8, PAIR), 0
                )


def conv_backward(parts, grad_parts, weight):
    frames, channels = parts[1].shape
    out, taps = pl.pallas_call(
        conv_backward_kernel,
        out_shape=[
            jax.ShapeDtypeStruct((frames, channels), jnp.float32),
            jax.ShapeDtypeStruct((8 * KERNEL, channels), jnp.float32),
        ],
        in_specs=[pl.BlockSpec(memory_space=pltpu.VMEM)] * 7,
        out_specs=[pl.BlockSpec(memory_space=pltpu.VMEM)] * 2,
        scratch_shapes=[pltpu.VMEM((frames + 32, channels), jnp.float32)] * 2,
        cost_estimate=pl.CostEstimate(
            flops=4 * KERNEL * frames * channels,
            bytes_accessed=8 * frames * channels,
            transcendentals=0,
        ),
        name="conv_backward",
    )(*parts, *grad_parts, weight)
    return (out, jnp.sum(taps.reshape(KERNEL, 8, channels), 1))


def group_sum_kernel(axes, sizes, x_ref, o_ref, slots, send_sem, recv_sem):
    places = [lax.axis_index(axis) for axis in axes]
    peers = []
    mine = 0
    for place, size in zip(places, sizes):
        mine = mine * size + place
    total = 1
    for size in sizes:
        total *= size
    for offset in range(1, total):
        rest, target = offset, {}
        for axis, place, size in reversed(list(zip(axes, places, sizes))):
            target[axis] = lax.rem(place + rest % size, size)
            rest //= size
        peers.append(target)
    barrier = pltpu.get_barrier_semaphore()
    for target in peers:
        pl.semaphore_signal(
            barrier, inc=1, device_id=target, device_id_type=pl.DeviceIdType.MESH
        )
    pl.semaphore_wait(barrier, total - 1)
    copies = []
    for number, target in enumerate(peers):
        copy = pltpu.make_async_remote_copy(
            src_ref=x_ref,
            dst_ref=slots.at[mine],
            send_sem=send_sem.at[number],
            recv_sem=recv_sem.at[number],
            device_id=target,
            device_id_type=pl.DeviceIdType.MESH,
        )
        copy.start()
        copies.append(copy)
    slots[mine] = x_ref[...]
    for copy in copies:
        copy.wait()
    result = slots[0]
    for number in range(1, total):
        result = result + slots[number]
    o_ref[...] = result


def group_sum(values, axes, number):
    sizes = [lax.axis_size(axis) for axis in axes]
    total = 1
    for size in sizes:
        total *= size
    return pl.pallas_call(
        functools.partial(group_sum_kernel, axes, sizes),
        out_shape=jax.ShapeDtypeStruct(values.shape, jnp.float32),
        in_specs=[pl.BlockSpec(memory_space=pltpu.VMEM)],
        out_specs=pl.BlockSpec(memory_space=pltpu.VMEM),
        scratch_shapes=[
            pltpu.VMEM((total,) + values.shape, jnp.float32),
            pltpu.SemaphoreType.DMA((total - 1,)),
            pltpu.SemaphoreType.DMA((total - 1,)),
        ],
        compiler_params=pltpu.CompilerParams(collective_id=number, has_side_effects=True),
        name="group_sum_" + str(number),
    )(values)


def flat_sum(arrays, stages):
    flat = jnp.concatenate([array.reshape(-1) for array in arrays])
    size = flat.shape[0]
    flat = jnp.pad(flat, (0, -size % 1024)).reshape(-1, 128)
    for axes, number in stages:
        flat = group_sum(flat, axes, number)
    flat = flat.reshape(-1)
    pieces, start = [], 0
    for array in arrays:
        pieces.append(lax.slice_in_dim(flat, start, start + array.size).reshape(array.shape))
        start += array.size
    return pieces


def gather_weights(*shards):
    rows = shards[0].shape[0]
    flat = jnp.concatenate([shard.reshape(rows, -1) for shard in shards], 1)
    part = rows // lax.axis_size("ctx")
    mine = lax.dynamic_slice_in_dim(flat, lax.axis_index("ctx") * part, part, 0)
    whole = lax.all_gather(mine, ("fsdp", "ctx"), axis=0, tiled=True)
    pieces, start = [], 0
    for shard in shards:
        width = shard.size // rows
        pieces.append(
            lax.slice_in_dim(whole, start, start + width, axis=1).reshape(-1, *shard.shape[1:])
        )
        start += width
    return pieces


def gather_both(up, down):
    part = up.shape[0] // lax.axis_size("ctx")
    start = lax.axis_index("ctx") * part
    mine = jnp.stack([lax.dynamic_slice_in_dim(shard, start, part, 0) for shard in (up, down)], 1)
    both = double(mine, "tp", 1, 2).reshape(part, -1)
    whole = lax.all_gather(both, ("fsdp", "ctx"), axis=0, tiled=True)
    middle = whole.shape[1] // 2
    return (whole[:, :middle], whole[:, middle:])


def reduce_both(part):
    own = halve(part.reshape(part.shape[0], 2, 2, -1), "tp", 1, 2)
    whole = double(double(own, "ctx", 2, 0), "ctx", 1, 1)
    whole = whole.reshape(-1, 2, own.shape[2]).astype(jnp.float32)
    return (whole[:, 0], whole[:, 1])


def pack_grads(*grads):
    return jnp.concatenate(
        [grad.astype(jnp.bfloat16).reshape(grad.shape[0], -1) for grad in grads], 1
    )


def reduce_grads(packed, *shapes):
    part = lax.psum_scatter(packed, ("fsdp", "ctx"), scatter_dimension=0, tiled=True)
    if lax.axis_size("ctx") == 4:
        whole = double(double(part, "ctx", 2, 0), "ctx", 1, 1).reshape(-1, part.shape[1])
    else:
        whole = lax.all_gather(part, "ctx", axis=0, tiled=True)
    pieces, start = [], 0
    for shape in shapes:
        width = 1
        for size in shape[1:]:
            width *= size
        pieces.append(
            lax.slice_in_dim(whole, start, start + width, axis=1)
            .astype(jnp.float32)
            .reshape(-1, *shape[1:])
        )
        start += width
    return pieces


def swap(values, axis, bit):
    return lax.ppermute(values, axis, [(i, i ^ bit) for i in range(lax.axis_size(axis))])


def halve(values, axis, bit, dim):
    own = lax.axis_index(axis) // bit % 2
    keep = lax.dynamic_index_in_dim(values, own, dim, keepdims=False)
    send = lax.dynamic_index_in_dim(values, 1 - own, dim, keepdims=False)
    other = swap(send, axis, bit)
    return (keep.astype(jnp.float32) + other.astype(jnp.float32)).astype(jnp.bfloat16)


def double(values, axis, bit, dim):
    own = lax.axis_index(axis) // bit % 2
    other = swap(values, axis, bit)
    return jnp.where(
        own == 0, jnp.stack([values, other], dim), jnp.stack([other, values], dim)
    )


def reduce_by_swaps(grad):
    if lax.axis_size("fsdp") != 4 or lax.axis_size("ctx") != 4:
        return reduce_grads(pack_grads(grad), (grad.shape[0],) + grad.shape[1:])[0]
    low = grad.astype(jnp.bfloat16).reshape(grad.shape[0], -1)
    total = low.reshape(2, 2, 2, 2, -1, low.shape[1])
    total = halve(total, "ctx", 1, 3)
    total = halve(total, "ctx", 2, 2)
    total = halve(total, "fsdp", 1, 1)
    total = halve(total, "fsdp", 2, 0)
    total = double(total, "ctx", 2, 0)
    total = double(total, "ctx", 1, 1)
    return total.astype(jnp.float32).reshape(-1, *grad.shape[1:])


def attend_plans(lengths, frames, chunk):
    me = lax.axis_index("ctx")
    return [
        jnp.stack(
            [lengths[0]]
            + [
                (me ^ block) * frames + start
                for block in blocks
                for start in range(0, frames, chunk)
            ]
        ).astype(jnp.int32)
        for blocks in ((0, 1), (2, 3))
    ]


def sum_by_swaps(arrays, axes):
    flat = jnp.concatenate([array.reshape(-1) for array in arrays])
    size = flat.shape[0]
    flat = jnp.pad(flat, (0, -size % 1024)).reshape(-1, 128)
    for axis in axes:
        bit = 1
        while bit < lax.axis_size(axis):
            flat = flat + swap(flat, axis, bit)
            bit *= 2
    flat = flat.reshape(-1)
    pieces, start = [], 0
    for array in arrays:
        pieces.append(lax.slice_in_dim(flat, start, start + array.size).reshape(array.shape))
        start += array.size
    return pieces


def product_rows(left, right):
    return lax.dot_general(
        left, right, (((1,), (1,)), ((), ())), preferred_element_type=jnp.float32
    )


def product_cols(left, right):
    return lax.dot_general(
        left, right, (((0,), (0,)), ((), ())), preferred_element_type=jnp.float32
    )


def feed_forward(stream, gain, weight_up, weight_down, total):
    normed, norm_back = jax.vjp(layer_norm, stream, gain)
    normed_low = normed.astype(jnp.bfloat16)
    hidden = jnp.dot(normed_low, weight_up, preferred_element_type=jnp.float32)
    active, active_back = jax.vjp(swish, hidden)
    active_low = active.astype(jnp.bfloat16)
    branch = total(product_rows(active_low, weight_down))
    return (branch, (norm_back, normed_low, active_back, active_low))


def feed_backward(branch_grad, saved, weight_up, weight_down, gain_early, total):
    norm_back, normed_low, active_back, active_low = saved
    grad_low = branch_grad.astype(jnp.bfloat16)
    down_grad = product_cols(grad_low, active_low)
    hidden_grad = active_back(jnp.dot(grad_low, weight_down, preferred_element_type=jnp.float32))[
        0
    ].astype(jnp.bfloat16)
    up_grad = product_cols(normed_low, hidden_grad)
    normed_part = product_rows(hidden_grad, weight_up)
    if not gain_early:
        stream_grad, gain_part = norm_back(total(normed_part))
        return (stream_grad, gain_part, up_grad, down_grad)
    _, gain_part = norm_back(normed_part)
    gain_part, normed_low_grad = lax.optimization_barrier(
        (gain_part, normed_part.astype(jnp.bfloat16))
    )
    stream_grad, _ = norm_back(total(normed_low_grad))
    return (stream_grad, gain_part, up_grad, down_grad)


def split_joined(joined, heads):
    width = heads * HEAD
    keys = joined[:, :width].reshape(joined.shape[0], heads, HEAD)
    values = joined[:, width:].reshape(joined.shape[0], heads, HEAD)
    return (keys, values)


def attend_scores(query, keys, length):
    scores = jnp.einsum("fhe,lhe->hfl", query, keys, preferred_element_type=jnp.float32)
    live_keys = jnp.arange(keys.shape[0]) < length
    return jnp.where(live_keys[None, None, :], scores, masked_score)


def attend_one(inputs):
    query, joined, length = inputs
    keys, values = split_joined(joined, query.shape[1])
    scores = attend_scores(query, keys, length)
    top = jnp.max(scores, -1, keepdims=True)
    raised = jnp.exp(scores - top)
    total = jnp.sum(raised, -1, keepdims=True)
    weights = (raised / total).astype(jnp.bfloat16)
    mixed = jnp.einsum("hfl,lhe->fhe", weights, values, preferred_element_type=jnp.float32)
    return (mixed.astype(jnp.bfloat16), (top + jnp.log(total))[..., 0])


def attend_back(inputs):
    query, joined, length, log_total, mixed_grad = inputs
    keys, values = split_joined(joined, query.shape[1])
    scores = attend_scores(query, keys, length)
    probs = jnp.exp(scores - log_total[..., None])
    probs_grad = jnp.einsum("fhe,lhe->hfl", mixed_grad, values, preferred_element_type=jnp.float32)
    center = jnp.sum(probs * probs_grad, -1, keepdims=True)
    score_grad = (probs * (probs_grad - center)).astype(jnp.bfloat16)
    query_grad = jnp.einsum("hfl,lhe->fhe", score_grad, keys, preferred_element_type=jnp.float32)
    keys_grad = jnp.einsum("hfl,fhe->lhe", score_grad, query, preferred_element_type=jnp.float32)
    values_grad = jnp.einsum(
        "hfl,fhe->lhe", probs.astype(jnp.bfloat16), mixed_grad, preferred_element_type=jnp.float32
    )
    frames_all = keys.shape[0]
    joined_grad = jnp.concatenate(
        [keys_grad.reshape(frames_all, -1), values_grad.reshape(frames_all, -1)], -1
    )
    return (query_grad, joined_grad)


def per_device(
    layer_input,
    out_grad,
    lengths,
    norm_gains,
    feed_up,
    feed_down,
    attend_in,
    attend_out,
    mixer_in,
    mixer_out,
    depth_kernel,
    batch_norm,
    final_up,
    final_down,
):
    batch, frames, width = layer_input.shape
    rows = batch * frames
    place = lax.axis_index("ctx") * frames + jnp.arange(frames, dtype=jnp.int32)
    live = (place[None, :] < lengths[:, None]).astype(jnp.float32)
    live_rows = live.reshape(rows, 1)
    live_cube = live[:, :, None]
    up_one, down_one = gather_weights(feed_up, feed_down)
    (proj_in,) = gather_weights(attend_in)
    proj_out, conv_in, conv_out = gather_weights(attend_out, mixer_in, mixer_out)
    stream = layer_input.reshape(rows, width)
    cotangent = out_grad.reshape(rows, width)
    branch_one, saved_one = feed_forward(
        stream, norm_gains[0], up_one, down_one, tensor_total
    )
    after_one = stream + 0.5 * branch_one
    normed, norm_back_two = jax.vjp(layer_norm, after_one, norm_gains[1])
    normed_two = normed.astype(jnp.bfloat16)
    projected = jnp.einsum("nd,dke->nke", normed_two, proj_in, preferred_element_type=jnp.float32)
    local_width = projected.shape[2]
    heads = local_width // HEAD
    split = projected.reshape(batch, frames, 3, heads, HEAD)

    def rotate_pair(query_raw, key_raw):
        return (rotary(query_raw, place) * HEAD ** (-0.5), rotary(key_raw, place))

    (query_rot, key_rot), rotate_back = jax.vjp(rotate_pair, split[:, :, 0], split[:, :, 1])
    query_low = query_rot.astype(jnp.bfloat16)
    joined = jnp.concatenate(
        [
            key_rot.astype(jnp.bfloat16).reshape(batch, frames, local_width),
            split[:, :, 2].astype(jnp.bfloat16).reshape(batch, frames, local_width),
        ],
        -1,
    )
    joined, late_up, late_down = lax.optimization_barrier((joined, final_up, final_down))
    by_frames = lax.axis_size("tp") == 2 and lax.axis_size("ctx") == 4
    if by_frames:
        up_two, down_two = gather_both(late_up, late_down)
    else:
        up_two, down_two = gather_weights(late_up, late_down)
    paired = local_width % PAIR == 0 and batch == 1 and lax.axis_size("ctx") == 4
    pairs = local_width // PAIR
    chunk = min(frames, 512)
    if paired:
        near_plan, far_plan = attend_plans(lengths, frames, chunk)
        query_rows = query_low.reshape(rows, local_width)
        owns = [
            jnp.concatenate(
                [joined[0, :, side * local_width + pair * PAIR :][:, :PAIR] for side in range(2)],
                1,
            )
            for pair in range(pairs)
        ]
        cores = [swap(own, "ctx", 1) for own in owns]
        chips = [swap(own, "ctx", 2) for own in owns]
        near_keys = [jnp.concatenate([own, core], 0) for own, core in zip(owns, cores)]
        far_keys, states, pair_out, pair_lse = [], [], [], []
        for pair in range(pairs):
            state = attend_forward(query_rows, pair, near_keys[pair], near_plan, chunk, ())
            near_plan, far_plan, chip, *state = lax.optimization_barrier(
                (near_plan, far_plan, chips[pair], *state)
            )
            states.append(state)
            far_keys.append(jnp.concatenate([chip, swap(chip, "ctx", 1)], 0))
        for pair in range(pairs):
            out, lse = attend_forward(
                query_rows, pair, far_keys[pair], far_plan, chunk, tuple(states[pair])
            )
            near_plan, far_plan, out, lse = lax.optimization_barrier(
                (near_plan, far_plan, out, lse)
            )
            pair_out.append(out)
            pair_lse.append(lse)
        mixed_rows = jnp.concatenate([out.astype(jnp.bfloat16).T for out in pair_out], 1)
    else:
        joined_all = lax.all_gather(joined, "ctx", axis=1, tiled=True)
        mixed, log_total = lax.map(attend_one, (query_low, joined_all, lengths))
        mixed_rows = mixed.reshape(rows, local_width)
    after_two = after_one + tensor_total(product_rows(mixed_rows, proj_out))
    normed, norm_back_three = jax.vjp(layer_norm, after_two, norm_gains[2])
    normed_three = normed.astype(jnp.bfloat16)
    gates = jnp.einsum("nd,dke->nke", normed_three, conv_in, preferred_element_type=jnp.float32)

    def gate_linear(values):
        return values[:, 0] * jax.nn.sigmoid(values[:, 1]) * live_rows

    gated, gate_back = jax.vjp(gate_linear, gates)
    channels = gated.shape[1]
    gated_low = gated.astype(jnp.bfloat16).reshape(batch, frames, channels)
    reach = KERNEL // 2
    conv_fused = batch == 1 and channels % PAIR == 0 and frames % 64 == 0
    if conv_fused:
        parts = halo_parts(gated_low[0], reach)
    else:
        padded = with_halo(gated_low, (("ctx", 1),), reach)
    if conv_fused:
        live_frames = lengths - lax.axis_index("ctx") * frames
        filtered, live_sum, live_square = conv_forward(parts, depth_kernel, live_frames)
        filtered = filtered[None]
    else:
        filtered = jnp.zeros((batch, frames, channels), jnp.float32)
        for offset in range(KERNEL):
            filtered = filtered + depth_kernel[offset] * padded[
                :, offset : offset + frames
            ].astype(jnp.float32)
        live_sum = jnp.sum(live_cube * filtered, (0, 1))
        live_square = jnp.sum(live_cube * filtered * filtered, (0, 1))
    live_count = jnp.full((channels,), jnp.sum(live))
    sums = flat_sum([live_sum, live_square, live_count], [(("fsdp", "ctx"), 0)])
    count = sums[2]
    mean = sums[0] / count
    variance = sums[1] / count - mean * mean
    rescale = lax.rsqrt(variance + norm_eps)
    unit = (filtered - mean) * rescale
    shifted = unit * batch_norm[0] + batch_norm[1]
    active, active_back = jax.vjp(swish, shifted.reshape(rows, channels))
    active_low = active.astype(jnp.bfloat16)
    conv_part = product_rows(active_low, conv_out)
    if by_frames:
        own_half = lax.axis_index("tp")

        def half_of(values):
            return lax.dynamic_slice_in_dim(values, own_half * (rows // 2), rows // 2, 0)

        conv_low = conv_part.astype(jnp.bfloat16).reshape(2, rows // 2, width)
        conv_send = lax.dynamic_index_in_dim(conv_low, 1 - own_half, 0, keepdims=False)
        conv_keep = lax.dynamic_index_in_dim(conv_low, own_half, 0, keepdims=False)
        conv_other = swap(conv_send, "tp", 1)
        after_three = (
            half_of(after_two) + conv_keep.astype(jnp.float32) + conv_other.astype(jnp.float32)
        )
        cotangent = half_of(cotangent)
        total = lambda values: values.astype(jnp.float32)
        share = 1.0
    else:
        after_three = after_two + tensor_total(conv_part)
        total = tensor_total
        share = 1.0 / lax.axis_size("tp")
    branch_four, saved_four = feed_forward(after_three, norm_gains[3], up_two, down_two, total)
    after_four = after_three + 0.5 * branch_four
    result, final_back = jax.vjp(layer_norm, after_four, norm_gains[4])
    grad_four, gain_five = final_back(cotangent)
    stream_grad, gain_four, up_two_grad, down_two_grad = feed_backward(
        0.5 * grad_four, saved_four, up_two, down_two, False, total
    )
    gain_four, gain_five = gain_four * share, gain_five * share
    grad_three = grad_four + stream_grad
    if by_frames:
        branch_low, result_low = lax.optimization_barrier(
            (grad_three.astype(jnp.bfloat16), result.astype(jnp.bfloat16))
        )
        branch_low = double(branch_low, "tp", 1, 0).reshape(rows, width)
        early, branch_low, result_low = lax.optimization_barrier(
            (pack_grads(up_two_grad, down_two_grad), branch_low, result_low)
        )
        result = double(result_low, "tp", 1, 0).astype(jnp.float32)
        grad_three = branch_low.astype(jnp.float32)
        both_part = lax.psum_scatter(early, ("fsdp", "ctx"), scatter_dimension=0, tiled=True)
    else:
        early, grad_three = lax.optimization_barrier(
            (pack_grads(up_two_grad, down_two_grad), grad_three)
        )
        up_two_grad, down_two_grad = reduce_grads(early, final_up.shape, final_down.shape)
        branch_low = grad_three.astype(jnp.bfloat16)
    conv_out_grad = product_cols(branch_low, active_low)
    shifted_grad = active_back(jnp.dot(branch_low, conv_out, preferred_element_type=jnp.float32))[
        0
    ].reshape(batch, frames, channels)
    bias_sum, scale_sum = flat_sum(
        [jnp.sum(shifted_grad, (0, 1)), jnp.sum(shifted_grad * unit, (0, 1))],
        [(("fsdp", "ctx"), 1)],
    )
    var_grad = -0.5 * rescale * rescale * batch_norm[0] * scale_sum
    first_grad = (-rescale * batch_norm[0] * bias_sum - 2.0 * mean * var_grad) / count
    second_grad = var_grad / count
    filtered_grad = (
        rescale * batch_norm[0] * shifted_grad
        + live_cube * (first_grad + 2.0 * filtered * second_grad)
    ).astype(jnp.bfloat16)
    if conv_fused:
        grad_parts = halo_parts(filtered_grad[0], reach)
        gated_grad, kernel_local = conv_backward(parts, grad_parts, depth_kernel)
    else:
        padded_grad = with_halo(filtered_grad, (("ctx", 1),), reach)
        filtered_wide = filtered_grad.astype(jnp.float32)
        gated_grad = jnp.zeros((batch, frames, channels), jnp.float32)
        kernel_terms = []
        for offset in range(KERNEL):
            start = 2 * reach - offset
            gated_grad = gated_grad + depth_kernel[offset] * padded_grad[
                :, start : start + frames
            ].astype(jnp.float32)
            kernel_terms.append(
                jnp.sum(filtered_wide * padded[:, offset : offset + frames].astype(jnp.float32), (0, 1))
            )
        kernel_local = jnp.stack(kernel_terms)
    gates_grad = gate_back(gated_grad.reshape(rows, channels))[0].astype(jnp.bfloat16)
    (kernel_total,) = sum_by_swaps([kernel_local], ("ctx", "fsdp"))
    conv_in_grad = jnp.einsum(
        "nd,nke->dke", normed_three, gates_grad, preferred_element_type=jnp.float32
    )
    normed_grad = tensor_total(
        jnp.einsum("nke,dke->nd", gates_grad, conv_in, preferred_element_type=jnp.float32)
    )
    stream_grad, gain_three = norm_back_three(normed_grad)
    share = 1.0 / lax.axis_size("tp")
    gain_three, gain_four, gain_five = sum_by_swaps(
        [gain_three * share, gain_four, gain_five], ("ctx", "fsdp", "tp")
    )
    grad_two = grad_three + stream_grad
    branch_low = grad_two.astype(jnp.bfloat16)
    proj_out_grad = product_cols(branch_low, mixed_rows)
    mixed_grad = (
        jnp.dot(branch_low, proj_out, preferred_element_type=jnp.float32)
        .astype(jnp.bfloat16)
        .reshape(batch, frames, heads, HEAD)
    )
    early = pack_grads(conv_in_grad, conv_out_grad, proj_out_grad)
    early, mixed_grad = lax.optimization_barrier((early, mixed_grad))
    conv_in_grad, conv_out_grad, proj_out_grad = reduce_grads(
        early, mixer_in.shape, mixer_out.shape, attend_out.shape
    )
    if paired:
        grad_rows = mixed_grad.reshape(rows, local_width)
        half = frames
        far_grads, far_parts, home, queries = [], [], [], []
        for pair in range(pairs):
            query_far, keys_far = attend_backward(
                query_rows, grad_rows, pair, far_keys[pair], far_plan,
                pair_lse[pair], pair_out[pair], chunk,
            )
            near_plan, far_plan, query_far, keys_far = lax.optimization_barrier(
                (near_plan, far_plan, query_far, keys_far)
            )
            queries.append(query_far)
            far_grads.append((keys_far[:half], swap(keys_far[half:], "ctx", 1)))
        for pair in range(pairs):
            one, other = far_grads[pair]
            part = (one.astype(jnp.float32) + other.astype(jnp.float32)).astype(jnp.bfloat16)
            near_plan, part = lax.optimization_barrier((near_plan, part))
            far_parts.append(swap(part, "ctx", 2))
            query_near, keys_near = attend_backward(
                query_rows, grad_rows, pair, near_keys[pair], near_plan,
                pair_lse[pair], pair_out[pair], chunk,
            )
            near_plan, query_near, keys_near = lax.optimization_barrier(
                (near_plan, query_near, keys_near)
            )
            queries[pair] = (queries[pair] + query_near).T
            home.append((keys_near[:half], swap(keys_near[half:], "ctx", 1)))
        home = [
            one.astype(jnp.float32) + other.astype(jnp.float32) + far.astype(jnp.float32)
            for (one, other), far in zip(home, far_parts)
        ]
        query_grad = jnp.concatenate(queries, 1).reshape(batch, frames, heads, HEAD)
        key_grad, value_grad = (
            jnp.concatenate([part[:, side * PAIR :][:, :PAIR] for part in home], 1).reshape(
                batch, frames, heads, HEAD
            )
            for side in range(2)
        )
    else:
        query_grad, joined_grad = lax.map(
            attend_back, (query_low, joined_all, lengths, log_total, mixed_grad)
        )
        joined_local = lax.psum_scatter(
            joined_grad.astype(jnp.bfloat16), "ctx", scatter_dimension=1, tiled=True
        ).astype(jnp.float32)
        key_grad = joined_local[..., :local_width].reshape(batch, frames, heads, HEAD)
        value_grad = joined_local[..., local_width:].reshape(batch, frames, heads, HEAD)
    query_raw_grad, key_raw_grad = rotate_back((query_grad, key_grad))
    proj_grad = (
        jnp.stack([query_raw_grad, key_raw_grad, value_grad], 2)
        .reshape(rows, 3, local_width)
        .astype(jnp.bfloat16)
    )
    normed_part = jnp.einsum(
        "nke,dke->nd", proj_grad, proj_in, preferred_element_type=jnp.float32
    ).astype(jnp.bfloat16)
    normed_part, proj_late = lax.optimization_barrier((normed_part, proj_grad))
    proj_in_grad = jnp.einsum(
        "nd,nke->dke", normed_two, proj_late, preferred_element_type=jnp.float32
    )
    normed_grad = tensor_total(normed_part)
    stream_grad, gain_two = norm_back_two(normed_grad)
    grad_one = grad_two + stream_grad
    if by_frames:
        grad_one, both_part = lax.optimization_barrier((grad_one, both_part))
        up_two_grad, down_two_grad = reduce_both(both_part)
    stream_grad, gain_one, up_one_grad, down_one_grad = feed_backward(
        0.5 * grad_one, saved_one, up_one, down_one, True, tensor_total
    )
    input_grad = grad_one + stream_grad
    share = 1.0 / lax.axis_size("tp")
    gain_one, gain_two = sum_by_swaps([gain_one, gain_two * share], ("ctx", "fsdp", "tp"))
    gain_total = jnp.stack([gain_one, gain_two, gain_three, gain_four, gain_five])
    proj_in_grad = reduce_by_swaps(proj_in_grad)
    down_one_grad = reduce_by_swaps(down_one_grad)
    up_one_grad = reduce_by_swaps(up_one_grad)
    return (
        result.reshape(batch, frames, width),
        input_grad.reshape(batch, frames, width),
        gain_total,
        up_one_grad,
        down_one_grad,
        proj_in_grad,
        proj_out_grad,
        conv_in_grad,
        conv_out_grad,
        kernel_total,
        jnp.stack([scale_sum, bias_sum]),
        up_two_grad,
        down_two_grad,
    )


def solution(mesh):
    placed = (
        P("fsdp", "ctx", None),
        P("fsdp", "ctx", None),
        P("fsdp"),
        P(),
        P("fsdp", "tp"),
        P("fsdp", "tp"),
        P("fsdp", None, "tp"),
        P("fsdp", "tp"),
        P("fsdp", None, "tp"),
        P("fsdp", "tp"),
        P(None, "tp"),
        P(None, "tp"),
        P("fsdp", "tp"),
        P("fsdp", "tp"),
    )
    return jax.shard_map(
        per_device,
        mesh=mesh,
        in_specs=placed,
        out_specs=(
            P("fsdp", "ctx", None),
            P("fsdp", "ctx", None),
            P(),
            P("fsdp", "tp"),
            P("fsdp", "tp"),
            P("fsdp", None, "tp"),
            P("fsdp", "tp"),
            P("fsdp", None, "tp"),
            P("fsdp", "tp"),
            P(None, "tp"),
            P(None, "tp"),
            P("fsdp", "tp"),
            P("fsdp", "tp"),
        ),
        check_vma=False,
    )
```
